256 devices in a mesh: gx: 16 (over z, core), gy: 4 (over y), gz: 4 (over x).
Axes of the slice: x: 4, y: 4, z: 8, core: 2. Of those that a mesh axis runs over, the one named last changes fastest.
Arguments:
- right_side: float32 [128, 64, 1024], P('gx', 'gy', 'gz'), may hold values from -8 to 8
- outer_diag: float32 [128, 64, 1024], P('gx', 'gy', 'gz'), may hold values from 0.25 to 2
- stencil_nodes: int32 [2097152], P(('gx', 'gy', 'gz')), may hold values from 0 to 28414
- stencil_weights: float32 [8, 2097152], P(None, ('gx', 'gy', 'gz')), may hold values from -4.2 to 4.2
- handover_dest: int32 [2097152, 1], P(('gx', 'gy', 'gz')), may hold values from 0 to 63; in each aligned block of 8192 rows (0 to 8191, 8192 to 16383, ...) at most 256 rows name the same one
- handover_cell: int32 [2097152], P(('gx', 'gy', 'gz')), may hold values from 0 to 65535
- pressure_prev: float32 [128, 128, 1024], P('gx', 'gy', 'gz'), may hold values from -6 to 6
- inner_source: float32 [128, 128, 1024], P('gx', 'gy', 'gz'), may hold values from -6 to 6
- inner_diag: float32 [128, 128, 1024], P('gx', 'gy', 'gz'), may hold values from 0.25 to 2
Outputs:
- solution_field: float32 [128, 64, 1024], P('gx', 'gy', 'gz')
- residual: float32 [128, 64, 1024], P('gx', 'gy', 'gz')
- pressure: float32 [128, 128, 1024], P('gx', 'gy', 'gz')
The draws below stay inside these ranges and needn't reach their ends.
Inputs may be any that keep to these rules, and one draw needn't show every extreme that they name: `handover_dest`: among the 8192 points of one device, at most 256 go to one destination, and some destination gets exactly 256.
All inputs are finite; a program needn't handle non-finite values.
Results may differ from the reference program's by a relative error of at most 0.00018.
Values sent between devices are 32-bit elements; how exact they have to be, the bound alone decides.
A program may use at most 64 MiB of HBM per device.

```python
import math
import jax
import jax.numpy as jnp
import numpy as np

CX = 8
CY = 16
CZ = 256
IX = 8
IY = 32
IZ = 256
HPTS = 8192
ITERS = 2
SWEEPS = 2
NODES = 8
CAP = 256
OX = 128
OY = 64
OZ = 1024
JX = 128
JY = 128
JZ = 1024
NPTS = 2097152
N_GX = 16
N_GY = 4
N_GZ = 4


def blockwise(key, lower, upper):
    levels = jax.random.uniform(key, (OX // CX, OY // CY, OZ // CZ), jnp.float32, lower, upper)
    levels = jnp.repeat(levels, CX, axis=0)
    levels = jnp.repeat(levels, CY, axis=1)
    return jnp.repeat(levels, CZ, axis=2)


def draw_right_side(key, part):
    subkeys = jax.random.split(jax.random.fold_in(key, 11), 5)
    index_x = jnp.arange(OX, dtype=jnp.int32)[:, None, None]
    index_y = jnp.arange(OY, dtype=jnp.int32)[None, :, None]
    index_z = jnp.arange(OZ, dtype=jnp.int32)[None, None, :]
    parity = ((index_x + index_y + index_z) % 2).astype(jnp.float32)
    checker = 1.0 - 2.0 * parity
    phases = jax.random.uniform(subkeys[0], (3,), jnp.float32, 0.0, 2.0 * math.pi)
    wave_x = jnp.sin(2.0 * math.pi * (index_x.astype(jnp.float32) + 0.5) / (4.0 * CX) + phases[0])
    wave_y = jnp.sin(2.0 * math.pi * (index_y.astype(jnp.float32) + 0.5) / (4.0 * CY) + phases[1])
    wave_z = jnp.sin(2.0 * math.pi * (index_z.astype(jnp.float32) + 0.5) / (4.0 * CZ) + phases[2])
    smooth = wave_x * wave_y * wave_z
    blend_level = blockwise(subkeys[1], 0.0, 1.0)
    magnitude = jax.random.uniform(subkeys[2], (OX, OY, OZ), jnp.float32, 0.5, 1.5)
    rough_part = checker * magnitude
    amplitude = jnp.exp(blockwise(subkeys[3], math.log(0.5), math.log(1.5)))
    noise_part = jnp.clip(jax.random.normal(subkeys[4], (OX, OY, OZ), jnp.float32), -3.0, 3.0)
    result_field = amplitude * (2.0 * blend_level * smooth + 1.5 * (1.0 - blend_level) * rough_part + 0.5 * noise_part)
    return result_field


def draw_outer_diag(key, part):
    subkeys = jax.random.split(jax.random.fold_in(key, 23), 2)
    block_level = jnp.exp(blockwise(subkeys[0], math.log(0.25), 0.0))
    factor = jax.random.uniform(subkeys[1], (OX, OY, OZ), jnp.float32, 1.0, 2.0)
    return jnp.clip(block_level * factor, 0.25, 2.0)


def with_ends(drawn, own_key, smallest, top_value):
    longest = drawn.shape.index(max(drawn.shape))
    spots = []
    for shift in (0, 1):
        where = [jax.random.randint(jax.random.fold_in(own_key, axis), (), 0, length) for axis, length in enumerate(drawn.shape)]
        where[longest] = (where[longest] + shift) % drawn.shape[longest]
        spots.append(tuple(where))
    return drawn.at[spots[0]].set(smallest).at[spots[1]].set(top_value)


def steps_of(own_key, shape, cuts, smallest, high):
    factor_of = 1.0
    for axis_at, shards_of in cuts:
        draws = jax.random.uniform(jax.random.fold_in(jax.random.fold_in(own_key, 6), axis_at), (shards_of,), jnp.float32, smallest / len(cuts), high / len(cuts))
        factor_of = factor_of * jnp.repeat(jnp.exp(draws), shape[axis_at] // shards_of).reshape((-1,) + (1,) * (len(shape) - 1 - axis_at))
    return factor_of


def assign_block(own_key, own, number, rows, count, top, most, skew):
    sequence = jax.random.permutation(own_key, count)
    crowded, usual = shares(count, rows * top, most, skew, True), shares(count, rows * top, most, skew, False)
    places = jnp.arange(count)

    def named(lengths, offset_by):
        used = int((lengths > 0).sum())
        fixed = max(1, used // 4)
        passed = fixed + (places - fixed + offset_by * (used - fixed)) % max(1, count - fixed)
        return jnp.zeros((count,), jnp.int32).at[sequence[jnp.where(places < fixed, places, passed)]].set(jnp.asarray(lengths, jnp.int32))

    lengths = jnp.where(number % 4 == 0, named(crowded, number // 4), named(usual, number - number // 4 - 1))
    mixed = jax.random.permutation(jax.random.fold_in(own, 3), count)
    giver, sink = mixed[0:count // 2 * 2:2], mixed[1:count // 2 * 2:2]
    margin = jnp.minimum(lengths[giver] - 1, most - lengths[sink]) // 2
    margin = jnp.where((giver == sequence[0]) | (sink == sequence[0]) | (lengths[sink] == 0), 0, jnp.maximum(margin, 0))
    passed = jax.random.randint(jax.random.fold_in(own, 4), (count // 2,), 0, 1 << 20) % (margin + 1)
    lengths = lengths.at[giver].add(-passed).at[sink].add(passed)
    labels = jnp.searchsorted(jnp.cumsum(lengths), jnp.arange(rows * top), side="right").astype(jnp.int32)
    grid = labels.reshape(top, rows).T
    grid = grid[jax.random.permutation(jax.random.fold_in(own, 1), rows)]
    offset_by = jax.random.randint(jax.random.fold_in(own, 2), (rows, 1), 0, top)
    return jnp.take_along_axis(grid, (jnp.arange(top)[None, :] + offset_by) % top, axis=1)


def shares(count, total, reach, lean, full):
    portions = [(1 << 20) // math.isqrt(grade ** lean) + 1 for grade in range(1, count + 1)]
    largest = reach if full else min(reach, max(-(-total // count), total * portions[0] // sum(portions)))
    least = 1 if total - largest >= count - 1 else 0
    counts, surplus = [largest] + [least] * (count - 1), total - largest - least * (count - 1)
    while surplus > 0:
        candidates = [i for i in range(1, count) if counts[i] < largest] or [i for i in range(1, count) if counts[i] < reach]
        mass, left = sum([portions[i] for i in candidates]), surplus
        for i in candidates:
            addition = min(reach - counts[i], max(1, left * portions[i] // mass), surplus)
            counts[i] = counts[i] + addition
            surplus = surplus - addition
    return np.array(counts)


def normal_values(own_key, dims, width, most, cuts=(), held_as=jnp.bfloat16):
    result = width * jax.random.normal(own_key, dims, jnp.float32)
    if cuts:
        result = result * steps_of(own_key, dims, cuts, -0.22, 0.18)
    return jnp.clip(result, -most, most).astype(held_as)


def setup_inputs(seed: int = 0) -> dict:
    key_list = jax.random.split(jax.random.key(seed), 10)
    right_side = draw_right_side(jax.random.fold_in(key_list[9], 71), 0)
    outer_diag = draw_outer_diag(jax.random.fold_in(key_list[9], 71), 0)
    stencil_nodes = with_ends(jax.random.randint(key_list[2], (NPTS,), 0, (CX - 1) * CY * CZ - CZ - 1), jax.random.fold_in(key_list[2], 1), 0, ((CX - 1) * CY * CZ - CZ - 1) - 1).astype(jnp.int32)
    stencil_weights = normal_values(key_list[3], (NODES, NPTS), 0.7, 4.2, ((1, 256),), jnp.float32)
    handover_dest_keys = jax.random.split(jax.random.fold_in(key_list[4], 1), NPTS // HPTS)
    handover_dest_turns = jax.random.permutation(jax.random.fold_in(key_list[4], 3), NPTS // HPTS)
    handover_dest = jax.vmap(lambda own, number: assign_block(jax.random.fold_in(key_list[4], 2), own, number, HPTS, N_GX * N_GY, 1, CAP, 2))(handover_dest_keys, handover_dest_turns).reshape((NPTS, 1))
    handover_cell = with_ends(jax.random.randint(key_list[5], (NPTS,), 0, IX * IY * IZ), jax.random.fold_in(key_list[5], 1), 0, (IX * IY * IZ) - 1).astype(jnp.int32)
    pressure_prev = normal_values(key_list[6], (JX, JY, JZ), 1.0, 6.0, ((0, 16), (1, 4), (2, 4)), jnp.float32)
    inner_source = normal_values(key_list[7], (JX, JY, JZ), 1.0, 6.0, ((0, 16), (1, 4), (2, 4)), jnp.float32)
    inner_diag = jnp.clip(0.25 + 1.75 * jax.random.uniform(key_list[8], (JX, JY, JZ), jnp.float32) ** steps_of(key_list[8], (JX, JY, JZ), ((0, 16), (1, 4), (2, 4)), -0.2, 0.2), 0.25, 2.0)
    return dict(right_side=right_side, outer_diag=outer_diag, stencil_nodes=stencil_nodes, stencil_weights=stencil_weights, handover_dest=handover_dest, handover_cell=handover_cell, pressure_prev=pressure_prev, inner_source=inner_source, inner_diag=inner_diag)


def neighbours(field):
    padded = jnp.pad(field, 1)
    total = padded[2:, 1:-1, 1:-1] + padded[:-2, 1:-1, 1:-1]
    total = total + padded[1:-1, 2:, 1:-1] + padded[1:-1, :-2, 1:-1]
    total = total + padded[1:-1, 1:-1, 2:] + padded[1:-1, 1:-1, :-2]
    return total


def reference(right_side, outer_diag, stencil_nodes, stencil_weights, handover_dest, handover_cell, pressure_prev, inner_source, inner_diag):
    solution_field = jnp.zeros_like(right_side)
    residual, direction = right_side, right_side
    norm_now = jnp.sum(residual * residual)
    for step in range(ITERS):
        image = (6.0 + outer_diag) * direction - neighbours(direction)
        alpha = norm_now / jnp.sum(direction * image)
        solution_field = solution_field + alpha * direction
        residual = residual - alpha * image
        norm_next = jnp.sum(residual * residual)
        direction = residual + (norm_next / norm_now) * direction
        norm_now = norm_next
    count = stencil_nodes.shape[0]
    point = jnp.arange(count, dtype=jnp.int32)
    device = point // HPTS
    block_x = device // (N_GY * N_GZ)
    block_y = (device // N_GZ) % N_GY
    block_z = device % N_GZ
    corner = jnp.arange(NODES, dtype=jnp.int32)
    offsets = ((corner // 4) % 2) * (CY * CZ) + ((corner // 2) % 2) * CZ + corner % 2
    nodes = stencil_nodes[None, :] + offsets[:, None]
    local_a = nodes // (CY * CZ)
    local_b = (nodes // CZ) % CY
    local_c = nodes % CZ
    global_node = ((block_x * CX + local_a) * (CY * N_GY) + block_y * CY + local_b) * (CZ * N_GZ) + block_z * CZ + local_c
    sampled = solution_field.reshape(-1)[global_node.astype(jnp.int32)]
    handed = jnp.sum(stencil_weights * sampled, axis=0)
    dest = handover_dest[:, 0]
    dest_x = dest // N_GY
    dest_y = dest % N_GY
    cell_a = handover_cell // (IY * IZ)
    cell_b = (handover_cell // IZ) % IY
    cell_c = handover_cell % IZ
    target = ((dest_x * IX + cell_a) * (IY * N_GY) + dest_y * IY + cell_b) * (IZ * N_GZ) + block_z * IZ + cell_c
    rhs = inner_source.reshape(-1).at[target.astype(jnp.int32)].add(handed).reshape(inner_source.shape)
    pressure = pressure_prev
    for sweep in range(SWEEPS):
        pressure = (rhs + neighbours(pressure)) / (6.0 + inner_diag)
    return solution_field, residual, pressure
```

```python
import functools

import jax
import jax.numpy as jnp
from jax import lax
from jax.experimental import pallas as pl
from jax.experimental.pallas import tpu as pltpu
from jax.sharding import PartitionSpec as P

MESH = pl.DeviceIdType.MESH
F32 = jnp.float32
BF16 = jnp.bfloat16
I32 = jnp.int32
LANE = 128
BLK = 256


def iota(shape, dim):
    return lax.broadcasted_iota(I32, shape, dim)


def halves(x):
    hi = x.astype(BF16).astype(F32)
    return hi, x - hi


def nt(a, b):
    return lax.dot_general(a, b, (((1,), (1,)), ((), ())), preferred_element_type=F32)


def nn(a, b):
    return lax.dot_general(a, b, (((1,), (0,)), ((), ())), preferred_element_type=F32)


def two_sum(a, b):
    s = a + b
    t = s - a
    return s, (a - (s - t)) + (b - t)


def two_prod(a, b):
    p = a * b
    ca, cb = 4097.0 * a, 4097.0 * b
    ah, bh = ca - (ca - a), cb - (cb - b)
    al, bl = a - ah, b - bh
    return p, ((ah * bh - p) + ah * bl + al * bh) + al * bl


def dd_times(x, f):
    p, e = two_prod(x[0], f)
    return two_sum(p, e + x[1] * f)


def dd_add(x, y):
    s, e = two_sum(x[0], y[0])
    return two_sum(s, e + (x[1] + y[1]))


def column(v, at):
    groups = v.shape[0] // 8
    tile = at // LANE * LANE
    lanes = v[:, tile : tile + LANE].reshape(groups, 8, LANE)
    spread = jnp.broadcast_to(lanes[:, :, at - tile : at - tile + 1], (groups, 8, LANE))
    keep = iota((groups, 8, LANE), 2) == iota((groups, 8, LANE), 0)
    return jnp.sum(jnp.where(keep, spread, 0.0), axis=0)


def uncolumn(c, rows):
    groups = rows // 8
    keep = iota((groups, 8, LANE), 2) == iota((groups, 8, LANE), 0)
    picked = jnp.where(keep, jnp.broadcast_to(c[None], (groups, 8, LANE)), 0.0)
    return jnp.sum(picked, axis=2, keepdims=True).reshape(rows, 1)


def neighbour_sum(v, halo_x, halo_y, halo_z, at_ends):
    rows, nz = v.shape
    ny = halo_x.shape[1]
    planes = rows // ny
    first_x, last_x, first_y, last_y, first_z, last_z = at_ends
    low = jnp.where(first_x, 0.0, halo_x[0])
    high = jnp.where(last_x, 0.0, halo_x[1])
    total = jnp.concatenate([low, v[: rows - ny]], axis=0)
    total = total + jnp.concatenate([v[ny:], high], axis=0)
    in_plane = iota((rows, nz), 0) % ny

    def rows_of(h):
        return jnp.broadcast_to(h[:, None, :], (planes, ny, nz)).reshape(rows, nz)

    low = rows_of(jnp.where(first_y, 0.0, halo_y[0]))
    high = rows_of(jnp.where(last_y, 0.0, halo_y[1]))
    total = total + jnp.where(in_plane == 0, low, pltpu.roll(v, 1, 0))
    total = total + jnp.where(in_plane == ny - 1, high, pltpu.roll(v, rows - 1, 0))
    lane = iota((rows, nz), 1)
    low = uncolumn(jnp.where(first_z, 0.0, halo_z[0]), rows)
    high = uncolumn(jnp.where(last_z, 0.0, halo_z[1]), rows)
    total = total + jnp.where(lane == 0, low, pltpu.roll(v, 1, 1))
    total = total + jnp.where(lane == nz - 1, high, pltpu.roll(v, nz - 1, 1))
    return total


def kernel(
    sizes,
    right_hbm, odiag_hbm, nodes_hbm, weights_hbm, dest_hbm, cell_hbm, prev_hbm, source_hbm, idiag_hbm,
    x_hbm, res_hbm, p_hbm,
    right, odiag, nodes, weights, dest, cell, prev, source, idiag, load_sem,
    q0, q1, p1, x_out, res_out, p_out, store_sem,
    hx_o, hy_o, hz_o, sy_o, sz_o, hx_i, hy_i, hz_i, sy_i, sz_i, halo_send, halo_recv,
    ar1, ar2, ar_send, ar_recv,
    tx, rx, tx_cells, rx_cells, a2a_send, a2a_recv,
    rank_hot, dest_hot, carry, cells_acc, col_hot, row_weight, handed,
    cell_row, cell_col, acc,
):
    ngx, ngy, ngz, cy, iy = sizes
    mx, my, mz = lax.axis_index("gx"), lax.axis_index("gy"), lax.axis_index("gz")
    groups = ngx * ngy
    me = mx * ngy + my
    points = nodes.shape[1]
    blocks = points // BLK
    cap = tx.shape[2]
    at_ends = (mx == 0, mx == ngx - 1, my == 0, my == ngy - 1, mz == 0, mz == ngz - 1)

    loads = []
    for i, (a, b) in enumerate(
        ((right_hbm, right), (dest_hbm, dest), (cell_hbm, cell), (odiag_hbm, odiag), (prev_hbm, prev),
         (nodes_hbm, nodes), (weights_hbm, weights), (source_hbm, source), (idiag_hbm, idiag))
    ):
        c = pltpu.make_async_copy(a, b, load_sem.at[i])
        c.start()
        loads.append(c)

    barrier = pltpu.get_barrier_semaphore()

    def peer(k):
        t = lax.rem(me + k, groups)
        return t, (t // ngy, lax.rem(t, ngy), mz)

    def side(k):
        t = lax.rem(my * ngz + mz + k, ngy * ngz)
        return t, (mx, t // ngz, lax.rem(t, ngz))

    def greet_peer(k, _):
        pl.semaphore_signal(barrier, inc=1, device_id=peer(k)[1], device_id_type=MESH)
        return 0

    lax.fori_loop(1, groups, greet_peer, 0)

    def greet_layer(k, _):
        z = lax.rem(mz + 1 + k // ngy, ngz)
        pl.semaphore_signal(barrier, inc=1, device_id=(mx, lax.rem(k, ngy), z), device_id_type=MESH)
        return 0

    lax.fori_loop(0, (ngz - 1) * ngy, greet_layer, 0)
    for c in loads[:1]:
        c.wait()
    pl.semaphore_wait(barrier, groups - 1 + (ngz - 1) * ngy)

    up = ((lax.rem(mx + 1, ngx), my, mz), (mx, lax.rem(my + 1, ngy), mz), (mx, my, lax.rem(mz + 1, ngz)))
    down = (
        (lax.rem(mx + ngx - 1, ngx), my, mz),
        (mx, lax.rem(my + ngy - 1, ngy), mz),
        (mx, my, lax.rem(mz + ngz - 1, ngz)),
    )

    def send_halo(which, src, hx, hy, hz, sy, sz, slot):
        rows, nz = src.shape
        ny = hx.shape[2]
        planes = rows // ny
        copies = []

        def send(j, a, b, to):
            c = pltpu.make_async_remote_copy(
                a, b, halo_send.at[which, j], halo_recv.at[which, j], device_id=to, device_id_type=MESH
            )
            c.start()
            copies.append(c)

        send(0, src.at[pl.ds(rows - ny, ny)], hx.at[slot, 0], up[0])
        send(1, src.at[pl.ds(0, ny)], hx.at[slot, 1], down[0])
        v = src[...]
        solid = v.reshape(planes, ny, nz)
        sy[slot, 0] = solid[:, ny - 1, :]
        sy[slot, 1] = solid[:, 0, :]
        send(2, sy.at[slot, 0], hy.at[slot, 0], up[1])
        send(3, sy.at[slot, 1], hy.at[slot, 1], down[1])
        sz[slot, 0] = column(v, nz - 1)
        sz[slot, 1] = column(v, 0)
        send(4, sz.at[slot, 0], hz.at[slot, 0], up[2])
        send(5, sz.at[slot, 1], hz.at[slot, 1], down[2])
        return copies

    outer = (hx_o, hy_o, hz_o, sy_o, sz_o)
    inner = (hx_i, hy_i, hz_i, sy_i, sz_i)
    unsent = []
    first = send_halo(0, right, *outer, 0)
    loads[4].wait()
    prev_halo = send_halo(1, prev, *inner, 0)

    loads[1].wait()
    loads[2].wait()
    tri = jnp.concatenate(
        [
            jnp.where(iota((BLK, BLK), 0) < iota((BLK, BLK), 1), 1.0, 0.0),
            jnp.ones((BLK, BLK), F32),
        ],
        axis=1,
    ).astype(BF16)
    carry[...] = jnp.zeros_like(carry)
    step = 8 if blocks % 8 == 0 else 1
    group_id = iota((groups, BLK), 0)
    slot_id = iota((cap, BLK), 0).astype(F32)

    def rank_step(j, _):
        base = pl.multiple_of(j * step * BLK, BLK)
        names = dest[:, pl.ds(base, step * BLK)]
        hots = [
            jnp.where(group_id == names[:, b * BLK : (b + 1) * BLK], 1.0, 0.0)
            for b in range(step)
        ]
        counts = nn(jnp.concatenate(hots, axis=0).astype(BF16), tri)
        seen = carry[...]
        for b in range(step):
            part = counts[b * groups : (b + 1) * groups]
            rank = jnp.sum(hots[b] * (part[:, :BLK] + seen), axis=0, keepdims=True)
            seen = seen + part[:, BLK:]
            at = pl.ds(pl.multiple_of(base + b * BLK, BLK), BLK)
            rank_hot[:, at] = jnp.where(slot_id == rank, 1.0, 0.0).astype(BF16)
            dest_hot[:, at] = hots[b].astype(BF16)
        carry[...] = seen
        return 0

    lax.fori_loop(0, blocks // step, rank_step, 0)

    wide = min(points, 2048)

    cells_acc[...] = jnp.zeros_like(cells_acc)

    def cells_step(j, _):
        at = pl.ds(pl.multiple_of(j * wide, wide), wide)
        c = cell[:, at]
        hot = dest_hot[:, at].astype(F32)
        left = jnp.concatenate([hot * (c // 256).astype(F32), hot * (c % 256).astype(F32)], axis=0).astype(BF16)
        cells_acc[...] += nt(left, rank_hot[:, at])
        return 0

    lax.fori_loop(0, points // wide, cells_step, 0)
    both = cells_acc[...]
    tx_cells[...] = (both[:groups] * 256.0 + both[groups:]).astype(I32).reshape(groups, 1, cap)

    def exchange(src, dst, which):
        def go(k, _):
            t, to = peer(k)
            pltpu.make_async_remote_copy(
                src.at[t], dst.at[me], a2a_send.at[which], a2a_recv.at[which], device_id=to, device_id_type=MESH
            ).start()
            return 0

        lax.fori_loop(1, groups, go, 0)
        dst[pl.ds(me, 1)] = src[pl.ds(me, 1)]

    def exchanged(src, dst, which):
        many = pl.ds(0, groups - 1)
        pltpu.make_async_copy(dst.at[many], dst.at[many], a2a_recv.at[which]).wait()

    def exchange_sent(src, dst, which):
        many = pl.ds(0, groups - 1)
        pltpu.make_async_copy(src.at[many], src.at[many], a2a_send.at[which]).wait()

    exchange(tx_cells, rx_cells, 0)

    for c in first:
        c.wait_recv()
    loads[3].wait()
    r = right[...]
    diag = 6.0 + odiag[...]
    q0[...] = diag * r - neighbour_sum(r, hx_o[0], hy_o[0], hz_o[0], at_ends)
    second = send_halo(2, q0, *outer, 1)

    loads[5].wait()
    loads[6].wait()
    nz = right.shape[1]
    row_id = iota((right.shape[0], BLK), 0)
    col_id = iota((nz, BLK), 0)

    def weigh(j, _):
        at = pl.ds(pl.multiple_of(j * BLK, BLK), BLK)
        n = nodes[:, at]
        off = row_id - n // nz
        w = weights[:, at]
        hits = (off == 0, off == 1, off == cy, off == cy + 1)
        for dc in range(2):
            total = jnp.zeros(off.shape, F32)
            for hit, k in zip(hits, (0, 2, 4, 6)):
                total = jnp.where(hit, w[k + dc : k + dc + 1], total)
            row_weight[pl.ds(dc * off.shape[0], off.shape[0]), at] = total
        col_hot[:, at] = jnp.where(col_id == n % nz, 1.0, 0.0).astype(BF16)
        return 0

    lax.fori_loop(0, blocks // 2, weigh, 0)

    for c in second:
        c.wait_recv()
    q = q0[...]
    qq = diag * q - neighbour_sum(q, hx_o[1], hy_o[1], hz_o[1], at_ends)
    q1[...] = qq
    row8 = iota((8, LANE), 0)
    packed = jnp.zeros((8, LANE), F32)
    for k, (a, b) in enumerate(((r, r), (r, q), (q, q), (q, qq))):
        s = jnp.sum((a * b).reshape(-1, 8, nz), axis=0)
        t = s[:, :LANE]
        for m in range(LANE, nz, LANE):
            t = t + s[:, m : m + LANE]
        packed = jnp.where(row8 == k, jnp.sum(t, axis=0, keepdims=True), packed)
    packed = jnp.broadcast_to(jnp.sum(packed, axis=1, keepdims=True), (8, LANE))

    def all_to_one(value, buf, n, mine, partner, which):
        buf[pl.ds(mine, 1)] = value[None]

        def go(k, _):
            pltpu.make_async_remote_copy(
                buf.at[mine], buf.at[mine], ar_send.at[which], ar_recv.at[which],
                device_id=partner(k), device_id_type=MESH,
            ).start()
            return 0

        lax.fori_loop(1, n, go, 0)

    def all_arrived(buf, n, which):
        many = pl.ds(0, n - 1)
        pltpu.make_async_copy(buf.at[many], buf.at[many], ar_recv.at[which]).wait()
        s, e = buf[0], jnp.zeros((8, LANE), F32)
        for i in range(1, n):
            s, d = two_sum(s, buf[i])
            e = e + d
        return s + jnp.where(row8 >= 4, pltpu.roll(e, 4, 0), 0.0)

    def all_sent(buf, n, which):
        many = pl.ds(0, n - 1)
        pltpu.make_async_copy(buf.at[many], buf.at[many], ar_send.at[which]).wait()

    all_to_one(packed, ar1, ngx, mx, lambda k: (lax.rem(mx + k, ngx), my, mz), 0)
    lax.fori_loop(blocks // 2, blocks, weigh, 0)
    packed = all_arrived(ar1, ngx, 0)
    all_to_one(packed, ar2, ngy * ngz, my * ngz + mz, lambda k: side(k)[1], 1)

    for c in prev_halo:
        c.wait_recv()
    loads[7].wait()
    loads[8].wait()
    p1[...] = source[...] + neighbour_sum(prev[...], hx_i[0], hy_i[0], hz_i[0], at_ends)
    exchanged(tx_cells, rx_cells, 0)
    nzi = source.shape[1]
    in_row = iota((source.shape[0], cap), 0)
    in_col = iota((nzi, cap), 0)

    def place(s, _):
        c = rx_cells[s]
        at = pl.ds(pl.multiple_of(s * cap, LANE), cap)
        cell_row[:, at] = jnp.where(in_row == c // nzi, 1.0, 0.0).astype(BF16)
        cell_col[:, at] = jnp.where(in_col == c % nzi, 1.0, 0.0).astype(BF16)
        return 0

    lax.fori_loop(0, groups // 2, place, 0)

    mu_rows = all_arrived(ar2, ngy * ngz, 1)
    mu = [(mu_rows[k : k + 1], mu_rows[4 + k : 5 + k]) for k in range(4)]
    a0 = mu[0][0] / mu[1][0]
    two_a0 = 2.0 * a0
    rr1 = dd_add(mu[0], dd_times(dd_add(dd_times(mu[2], a0), (-2.0 * mu[1][0], -2.0 * mu[1][1])), a0))
    rr1 = rr1[0] + rr1[1]
    beta = rr1 / mu[0][0]
    g = 1.0 + beta
    m2 = dd_times(mu[2], -two_a0)
    curve = dd_times(dd_add(dd_times(mu[1], g), m2), g)
    curve = dd_add(curve, dd_times(dd_times(mu[3], a0), a0))
    a1 = rr1 / (curve[0] + curve[1])
    a0, a1, beta = a0[:, :1], a1[:, :1], beta[:, :1]
    r = right[...]
    q = q0[...]
    r1 = r - a0 * q
    d1 = r1 + beta * r
    x = a0 * r + a1 * d1
    x_out[...] = x
    res_out[...] = r1 - a1 * ((q - a0 * q1[...]) + beta * q)
    stores = [
        pltpu.make_async_copy(x_out, x_hbm, store_sem.at[0]),
        pltpu.make_async_copy(res_out, res_hbm, store_sem.at[1]),
    ]
    for c in stores:
        c.start()

    nr = x.shape[0]
    ahead = pltpu.roll(x, nz - 1, 1)
    ahead = jnp.where(iota((nr, nz), 1) == nz - 1, pltpu.roll(ahead, nr - 1, 0), ahead)
    field = jnp.concatenate([x, ahead], axis=0)
    hi, lo = halves(field)
    field = jnp.concatenate([hi, lo], axis=0).astype(BF16)
    mid = 4 if blocks % 4 == 0 else 1

    def sample(j, _):
        for b in range(mid):
            at = pl.ds(pl.multiple_of((j * mid + b) * BLK, BLK), BLK)
            got = nn(field, col_hot[:, at])
            got = (got[: 2 * nr] + got[2 * nr :]) * row_weight[:, at]
            handed[:, at] = jnp.sum(got, axis=0, keepdims=True)
        return 0

    lax.fori_loop(0, blocks // mid, sample, 0)

    acc[pl.ds(0, 2 * groups)] = jnp.zeros((2 * groups, cap), F32)

    def route(j, _):
        at = pl.ds(pl.multiple_of(j * wide, wide), wide)
        h_hi, h_lo = halves(handed[:, at])
        hot = dest_hot[:, at].astype(F32)
        left = jnp.concatenate([hot * h_hi, hot * h_lo], axis=0).astype(BF16)
        acc[pl.ds(0, 2 * groups)] += nt(left, rank_hot[:, at])
        return 0

    lax.fori_loop(0, points // wide, route, 0)
    tx[...] = (acc[pl.ds(0, groups)] + acc[pl.ds(groups, groups)]).reshape(groups, 1, cap)
    exchange(tx, rx, 1)
    lax.fori_loop(groups // 2, groups, place, 0)
    acc[...] = jnp.zeros_like(acc)
    inv = 1.0 / (6.0 + idiag[...])
    exchanged(tx, rx, 1)

    ni = source.shape[0]
    batch = 8 if groups % 8 == 0 else groups

    def gather_in(j, _):
        at = pl.ds(pl.multiple_of(j * batch * cap, LANE), batch * cap)
        val = jnp.concatenate([rx[j * batch + b] for b in range(batch)], axis=1)
        v_hi, v_lo = halves(val)
        rows = cell_row[:, at]
        left = jnp.concatenate([rows * v_hi.astype(BF16), rows * v_lo.astype(BF16)], axis=0)
        acc[...] += nt(left, cell_col[:, at])
        return 0

    lax.fori_loop(0, groups // batch, gather_in, 0)
    added = acc[pl.ds(0, ni)] + acc[pl.ds(ni, ni)]
    p = (p1[...] + added) * inv
    p1[...] = p
    last = send_halo(3, p1, *inner, 1)
    rhs = source[...] + added
    for c in last:
        c.wait_recv()
    p_out[...] = (rhs + neighbour_sum(p, hx_i[1], hy_i[1], hz_i[1], at_ends)) * inv
    c = pltpu.make_async_copy(p_out, p_hbm, store_sem.at[2])
    c.start()
    stores.append(c)
    for c in first + prev_halo + second + last:
        c.wait_send()
    exchange_sent(tx_cells, rx_cells, 0)
    exchange_sent(tx, rx, 1)
    all_sent(ar1, ngx, 0)
    all_sent(ar2, ngy * ngz, 1)
    for c in stores:
        c.wait()


def solution(mesh):
    ngx, ngy, ngz = (mesh.shape[a] for a in ("gx", "gy", "gz"))
    groups = ngx * ngy

    def per_device(right, odiag, nodes, weights, dest, cell, prev, source, idiag):
        cx, cy, nz = right.shape
        ix, iy, nzi = source.shape
        points = nodes.shape[0]
        cap = 2 * points // groups
        no, ni = cx * cy, ix * iy
        v = pltpu.VMEM
        dma = pltpu.SemaphoreType.DMA
        scratch = [
            v((no, nz), F32), v((no, nz), F32), v((1, points), I32), v((8, points), F32), v((1, points), I32),
            v((1, points), I32), v((ni, nzi), F32), v((ni, nzi), F32), v((ni, nzi), F32), dma((9,)),
            v((no, nz), F32), v((no, nz), F32), v((ni, nzi), F32), v((no, nz), F32), v((no, nz), F32), v((ni, nzi), F32), dma((3,)),
            v((2, 2, cy, nz), F32), v((2, 2, cx, nz), F32), v((2, 2, 8, LANE), F32), v((2, 2, cx, nz), F32), v((2, 2, 8, LANE), F32),
            v((2, 2, iy, nzi), F32), v((2, 2, ix, nzi), F32), v((2, 2, 8, LANE), F32), v((2, 2, ix, nzi), F32), v((2, 2, 8, LANE), F32),
            dma((4, 6)), dma((4, 6)),
            v((ngx, 8, LANE), F32), v((ngy * ngz, 8, LANE), F32), dma((2,)), dma((2,)),
            v((groups, 1, cap), F32), v((groups, 1, cap), F32), v((groups, 1, cap), I32), v((groups, 1, cap), I32), dma((2,)), dma((2,)),
            v((cap, points), BF16), v((groups, points), BF16), v((groups, BLK), F32), v((2 * groups, cap), F32),
            v((nz, points), BF16), v((2 * no, points), F32), v((1, points), F32),
            v((ni, groups * cap), BF16), v((nzi, groups * cap), BF16), v((2 * ni, nzi), F32),
        ]
        x, res, p = pl.pallas_call(
            functools.partial(kernel, (ngx, ngy, ngz, cy, iy)),
            out_shape=(
                jax.ShapeDtypeStruct((no, nz), F32),
                jax.ShapeDtypeStruct((no, nz), F32),
                jax.ShapeDtypeStruct((ni, nzi), F32),
            ),
            in_specs=[pl.BlockSpec(memory_space=pl.ANY)] * 9,
            out_specs=[pl.BlockSpec(memory_space=pl.ANY)] * 3,
            scratch_shapes=scratch,
            compiler_params=pltpu.CompilerParams(
                collective_id=0, has_side_effects=True, vmem_limit_bytes=56 * 2**20
            ),
        )(
            right.reshape(no, nz), odiag.reshape(no, nz), nodes.reshape(1, points), weights,
            dest.reshape(1, points), cell.reshape(1, points), prev.reshape(ni, nzi),
            source.reshape(ni, nzi), idiag.reshape(ni, nzi),
        )
        return x.reshape(cx, cy, nz), res.reshape(cx, cy, nz), p.reshape(ix, iy, nzi)

    block = P("gx", "gy", "gz")
    every = ("gx", "gy", "gz")
    return jax.shard_map(
        per_device,
        mesh=mesh,
        in_specs=(block, block, P(every), P(None, every), P(every, None), P(every), block, block, block),
        out_specs=(block, block, block),
        check_vma=False,
    )
```

```python
import functools

import jax
import jax.numpy as jnp
from jax import lax
from jax.experimental import pallas as pl
from jax.experimental.pallas import tpu as pltpu
from jax.sharding import PartitionSpec as P

MESH = pl.DeviceIdType.MESH
F32 = jnp.float32
BF16 = jnp.bfloat16
I32 = jnp.int32
LANE = 128
BLK = 256


def iota(shape, dim):
    return lax.broadcasted_iota(I32, shape, dim)


def halves(x):
    hi = x.astype(BF16).astype(F32)
    return hi, x - hi


def nt(a, b):
    return lax.dot_general(a, b, (((1,), (1,)), ((), ())), preferred_element_type=F32)


def nn(a, b):
    return lax.dot_general(a, b, (((1,), (0,)), ((), ())), preferred_element_type=F32)


def two_sum(a, b):
    s = a + b
    t = s - a
    return s, (a - (s - t)) + (b - t)


def two_prod(a, b):
    p = a * b
    ca, cb = 4097.0 * a, 4097.0 * b
    ah, bh = ca - (ca - a), cb - (cb - b)
    al, bl = a - ah, b - bh
    return p, ((ah * bh - p) + ah * bl + al * bh) + al * bl


def dd_times(x, f):
    p, e = two_prod(x[0], f)
    return two_sum(p, e + x[1] * f)


def dd_add(x, y):
    s, e = two_sum(x[0], y[0])
    return two_sum(s, e + (x[1] + y[1]))


def column(v, at):
    groups = v.shape[0] // 8
    tile = at // LANE * LANE
    lanes = v[:, tile : tile + LANE].reshape(groups, 8, LANE)
    spread = jnp.broadcast_to(lanes[:, :, at - tile : at - tile + 1], (groups, 8, LANE))
    keep = iota((groups, 8, LANE), 2) == iota((groups, 8, LANE), 0)
    return jnp.sum(jnp.where(keep, spread, 0.0), axis=0)


def uncolumn(c, rows):
    groups = rows // 8
    keep = iota((groups, 8, LANE), 2) == iota((groups, 8, LANE), 0)
    picked = jnp.where(keep, jnp.broadcast_to(c[None], (groups, 8, LANE)), 0.0)
    return jnp.sum(picked, axis=2, keepdims=True).reshape(rows, 1)


def near_sum(v, ny):
    rows, nz = v.shape
    zero = jnp.zeros((ny, nz), F32)
    total = jnp.concatenate([zero, v[: rows - ny]], axis=0) + jnp.concatenate([v[ny:], zero], axis=0)
    in_plane = iota((rows, nz), 0) % ny
    lane = iota((rows, nz), 1)
    total = total + jnp.where(in_plane == 0, 0.0, pltpu.roll(v, 1, 0))
    total = total + jnp.where(in_plane == ny - 1, 0.0, pltpu.roll(v, rows - 1, 0))
    total = total + jnp.where(lane == 0, 0.0, pltpu.roll(v, 1, 1))
    return total + jnp.where(lane == nz - 1, 0.0, pltpu.roll(v, nz - 1, 1))


def far_sum(shape, halo_x, halo_y, halo_z, at_ends):
    rows, nz = shape
    ny = halo_x.shape[1]
    planes = rows // ny
    first_x, last_x, first_y, last_y, first_z, last_z = at_ends
    low = jnp.where(first_x, 0.0, halo_x[0])
    high = jnp.where(last_x, 0.0, halo_x[1])
    total = jnp.concatenate([low, jnp.zeros((rows - 2 * ny, nz), F32), high], axis=0)
    in_plane = iota((rows, nz), 0) % ny
    lane = iota((rows, nz), 1)

    def rows_of(h):
        return jnp.broadcast_to(h[:, None, :], (planes, ny, nz)).reshape(rows, nz)

    total = total + jnp.where(in_plane == 0, rows_of(jnp.where(first_y, 0.0, halo_y[0])), 0.0)
    total = total + jnp.where(in_plane == ny - 1, rows_of(jnp.where(last_y, 0.0, halo_y[1])), 0.0)
    total = total + jnp.where(lane == 0, uncolumn(jnp.where(first_z, 0.0, halo_z[0]), rows), 0.0)
    return total + jnp.where(lane == nz - 1, uncolumn(jnp.where(last_z, 0.0, halo_z[1]), rows), 0.0)


def field_of(x):
    nr, nz = x.shape
    ahead = pltpu.roll(x, nz - 1, 1)
    ahead = jnp.where(iota((nr, nz), 1) == nz - 1, pltpu.roll(ahead, nr - 1, 0), ahead)
    hi, lo = halves(jnp.concatenate([x, ahead], axis=0))
    return jnp.concatenate([hi, lo], axis=0).astype(BF16)


def hot_bf16(ids, wanted, value):
    return jnp.where(ids == wanted.astype(BF16), jnp.broadcast_to(value.astype(BF16), ids.shape), jnp.zeros(ids.shape, BF16))


def interpolate(field, n, w, cy, nz):
    nr = field.shape[0] // 4
    planes, parts, blk = nr // cy, cy // 8, n.shape[1]
    row = n // nz
    a0 = jnp.broadcast_to(row // cy, (8, blk))
    b0 = jnp.broadcast_to(row % cy, (8, blk))
    column_hot = hot_bf16(iota((nz, blk), 0).astype(BF16), n % nz, jnp.ones((1, blk), F32))
    got = nn(field, column_hot)
    got = got[: 2 * nr] + got[2 * nr :]
    here = [a0 == a for a in range(planes - 1)]

    def pick(dc, part, ahead):
        def at(a):
            s = dc * nr + min(a + ahead, planes - 1) * cy + part * 8
            return got[s : s + 8]

        v = at(planes - 2)
        for a in range(planes - 3, -1, -1):
            v = jnp.where(here[a], at(a), v)
        return v

    sub = iota((8, blk), 0)
    total = jnp.zeros((8, blk), F32)
    for dc in range(2):
        picked = [[pick(dc, part, ahead) for part in range(parts)] for ahead in range(2)] + [[pick(dc, 0, 2)]]
        for da in range(2):
            wa, wb = w(da * 4 + dc), w(da * 4 + 2 + dc)
            for part in range(parts):
                wt = jnp.where(b0 == sub + 8 * part, wa, jnp.where(b0 + 1 == sub + 8 * part, wb, 0.0))
                total = total + wt * picked[da][part]
            total = total + jnp.where(b0 + 1 == sub + cy, wb, 0.0) * picked[da + 1][0]
    return jnp.sum(total, axis=0, keepdims=True)


def kernel(
    sizes,
    right_hbm, odiag_hbm, nodes_hbm, weights_hbm, dest_hbm, cell_hbm, prev_hbm, source_hbm, idiag_hbm,
    x_hbm, res_hbm, p_hbm,
    right, odiag, nodes, weights, dest, cell, prev, source, idiag, load_sem,
    q0, q1, p1, x_out, res_out, p_out, store_sem,
    hx_o, hy_o, hz_o, sy_o, sz_o, hx_i, hy_i, hz_i, sy_i, sz_i, halo_send, halo_recv,
    ar1, ar2, ar_send, ar_recv,
    tx, rx, a2a_send, a2a_recv,
    rank, carry, field, handed_r, handed_q, routed, acc, inv,
):
    ngx, ngy, ngz, cy, iy = sizes
    mx, my, mz = lax.axis_index("gx"), lax.axis_index("gy"), lax.axis_index("gz")
    groups = ngx * ngy
    me = mx * ngy + my
    points = nodes.shape[1]
    blocks = points // BLK
    cap = tx.shape[2] // 3
    at_ends = (mx == 0, mx == ngx - 1, my == 0, my == ngy - 1, mz == 0, mz == ngz - 1)

    barrier = pltpu.get_barrier_semaphore()

    def peer(k):
        t = lax.rem(me + k, groups)
        return t, (t // ngy, lax.rem(t, ngy), mz)

    def greet_peer(k, _):
        pl.semaphore_signal(barrier, inc=1, device_id=peer(k)[1], device_id_type=MESH)
        return 0

    loads = []
    for i, (a, b) in enumerate(
        ((right_hbm, right), (dest_hbm, dest), (nodes_hbm, nodes), (weights_hbm, weights), (odiag_hbm, odiag),
         (cell_hbm, cell), (prev_hbm, prev), (source_hbm, source), (idiag_hbm, idiag))
    ):
        c = pltpu.make_async_copy(a, b, load_sem.at[i])
        c.start()
        loads.append(c)
    lax.fori_loop(1, groups, greet_peer, 0)
    side = [(a, b) for a in range(ngy) for b in range(ngz) if (a, b) != (0, 0)]
    side.sort(key=lambda t: -(min(t[0], ngy - t[0]) + min(t[1], ngz - t[1])))
    along = sorted(range(1, ngx), key=lambda k: -min(k, ngx - k))

    def beside(a, b):
        return (mx, lax.rem(my + a, ngy), lax.rem(mz + b, ngz))

    others = [(a, b) for a, b in side if b]
    for a, b in others:
        pl.semaphore_signal(barrier, inc=1, device_id=beside(a, b), device_id_type=MESH)

    up = ((lax.rem(mx + 1, ngx), my, mz), (mx, lax.rem(my + 1, ngy), mz), (mx, my, lax.rem(mz + 1, ngz)))
    down = (
        (lax.rem(mx + ngx - 1, ngx), my, mz),
        (mx, lax.rem(my + ngy - 1, ngy), mz),
        (mx, my, lax.rem(mz + ngz - 1, ngz)),
    )

    def pack_halo(src, sy, sz, ny, slot):
        rows, nz = src.shape
        v = src[...]
        solid = v.reshape(rows // ny, ny, nz)
        sy[slot, 0] = solid[:, ny - 1, :]
        sy[slot, 1] = solid[:, 0, :]
        sz[slot, 0] = column(v, nz - 1)
        sz[slot, 1] = column(v, 0)

    def send_halo(which, src, hx, hy, hz, sy, sz, slot):
        rows = src.shape[0]
        ny = hx.shape[2]
        copies = []

        def send(j, a, b, to):
            c = pltpu.make_async_remote_copy(
                a, b, halo_send.at[which, j], halo_recv.at[which, j], device_id=to, device_id_type=MESH
            )
            c.start()
            copies.append(c)

        send(0, src.at[pl.ds(rows - ny, ny)], hx.at[slot, 0], up[0])
        send(1, src.at[pl.ds(0, ny)], hx.at[slot, 1], down[0])
        send(2, sy.at[slot, 0], hy.at[slot, 0], up[1])
        send(3, sy.at[slot, 1], hy.at[slot, 1], down[1])
        send(4, sz.at[slot, 0], hz.at[slot, 0], up[2])
        send(5, sz.at[slot, 1], hz.at[slot, 1], down[2])
        return copies

    outer = (hx_o, hy_o, hz_o, sy_o, sz_o)
    inner = (hx_i, hy_i, hz_i, sy_i, sz_i)
    nz = right.shape[1]

    def rank_points():
        low = iota((BLK, BLK), 0) < iota((BLK, BLK), 1)
        tri = jnp.concatenate([jnp.where(low, 1.0, 0.0), jnp.ones((BLK, BLK), F32)], axis=1).astype(BF16)
        carry[...] = jnp.zeros_like(carry)
        step = next(s for s in (16, 4, 1) if blocks % s == 0)
        ids = iota((groups, BLK), 0)
        one = jnp.ones((1, BLK), F32)

        def rank_step(j, _):
            seen = carry[...]
            for b in range(step):
                at = pl.ds(pl.multiple_of((j * step + b) * BLK, BLK), BLK)
                name = dest[:, at]
                part = nn(hot_bf16(ids.astype(BF16), name, one), tri)
                rank[:, at] = jnp.sum(jnp.where(ids == name, part[:, :BLK] + seen, 0.0), axis=0, keepdims=True)
                seen = seen + part[:, BLK:]
            carry[...] = seen
            return 0

        lax.fori_loop(0, blocks // step, rank_step, 0)

    many = next(s for s in (16, 4, 1) if blocks % s == 0)

    def interpolate_all(handed, first, end):
        def go(j, _):
            for b in range(many):
                at = pl.ds(pl.multiple_of((j * many + b) * BLK, BLK), BLK)
                handed[:, at] = interpolate(field[...], nodes[:, at], lambda k: weights[k : k + 1, at], cy, nz)
            return 0

        lax.fori_loop(first, end, go, 0)

    def route():
        ids = iota((groups, BLK), 0).astype(BF16)
        slots = iota((cap, BLK), 0).astype(BF16)
        one = jnp.ones((1, BLK), F32)
        routed[...] = jnp.zeros_like(routed)

        def go(j, _):
            part = jnp.zeros(routed.shape, F32)
            for b in range(many):
                at = pl.ds(pl.multiple_of((j * many + b) * BLK, BLK), BLK)
                c = cell[:, at]
                values = (*halves(handed_r[:, at]), *halves(handed_q[:, at]), (c // 256).astype(F32), (c % 256).astype(F32))
                left = jnp.concatenate([hot_bf16(ids, dest[:, at], v) for v in values], axis=0)
                part = part + nt(left, hot_bf16(slots, rank[:, at], one))
            routed[...] += part
            return 0

        lax.fori_loop(0, blocks // many, go, 0)
        rows = [routed[pl.ds(i * groups, groups)] for i in range(6)]
        tx[...] = jnp.concatenate([rows[0] + rows[1], rows[2] + rows[3], rows[4] * 256.0 + rows[5]], axis=1).reshape(
            groups, 1, 3 * cap
        )

    middle = groups // 2

    def exchange(src, dst):
        def go(i, _):
            half = (i + 1) // 2
            t, to = peer(middle + jnp.where(lax.rem(i, 2) == 1, half, -half))
            pltpu.make_async_remote_copy(
                src.at[t], dst.at[me], a2a_send, a2a_recv, device_id=to, device_id_type=MESH
            ).start()
            return 0

        lax.fori_loop(0, groups - 1, go, 0)
        dst[pl.ds(me, 1)] = src[pl.ds(me, 1)]

    def exchanged(dst):
        all_but_one = pl.ds(0, groups - 1)
        pltpu.make_async_copy(dst.at[all_but_one], dst.at[all_but_one], a2a_recv).wait()

    def exchange_sent(src):
        all_but_one = pl.ds(0, groups - 1)
        pltpu.make_async_copy(src.at[all_but_one], src.at[all_but_one], a2a_send).wait()

    batch = next(s for s in (16, 8, 4, 2, 1) if groups % s == 0)
    ni, nzi = source.shape

    def scatter(c0, c1):
        rows_id = iota((ni, cap), 0).astype(BF16)
        cols_id = iota((nzi, cap), 0).astype(BF16)
        one = jnp.ones((1, cap), F32)
        acc[...] = jnp.zeros_like(acc)

        def go(j, _):
            part = jnp.zeros(acc.shape, F32)
            for b in range(batch):
                got = rx[j * batch + b]
                c = got[:, 2 * cap :].astype(I32)
                hi, lo = halves(c0 * got[:, :cap] + c1 * got[:, cap : 2 * cap])
                left = jnp.concatenate([hot_bf16(rows_id, c // nzi, hi), hot_bf16(rows_id, c // nzi, lo)], axis=0)
                part = part + nt(left, hot_bf16(cols_id, c % nzi, one))
            acc[...] += part
            return 0

        lax.fori_loop(0, groups // batch, go, 0)

    loads[0].wait()
    pack_halo(right, sy_o, sz_o, cy, 0)
    pl.semaphore_wait(barrier, groups - 1 + len(others))
    first = send_halo(0, right, *outer, 0)
    field[...] = field_of(right[...])
    loads[2].wait()
    loads[3].wait()
    interpolate_all(handed_r, 0, blocks // many)

    loads[4].wait()
    r = right[...]
    near = (6.0 + odiag[...]) * r - near_sum(r, cy)
    for c in first:
        c.wait_recv()
    q0[...] = near - far_sum(r.shape, hx_o[0], hy_o[0], hz_o[0], at_ends)
    pack_halo(q0, sy_o, sz_o, cy, 1)
    second = send_halo(2, q0, *outer, 1)
    field[...] = field_of(q0[...])
    loads[1].wait()
    rank_points()
    half = blocks // many // 2
    interpolate_all(handed_q, 0, half)

    q = q0[...]
    near = (6.0 + odiag[...]) * q - near_sum(q, cy)
    for c in second:
        c.wait_recv()
    q1[...] = near - far_sum(q.shape, hx_o[1], hy_o[1], hz_o[1], at_ends)
    row8 = iota((8, LANE), 0)
    packed = jnp.zeros((8, LANE), F32)
    r, qq = right[...], q1[...]
    for k, (a, b) in enumerate(((r, r), (r, q), (q, q), (q, qq))):
        s = jnp.sum((a * b).reshape(-1, 8, nz), axis=0)
        t = s[:, :LANE]
        for m in range(LANE, nz, LANE):
            t = t + s[:, m : m + LANE]
        packed = jnp.where(row8 == k, jnp.sum(t, axis=0, keepdims=True), packed)
    packed = jnp.broadcast_to(jnp.sum(packed, axis=1, keepdims=True), (8, LANE))

    def all_to_one(value, buf, mine, partners, which):
        buf[pl.ds(mine, 1)] = value[None]
        for to in partners:
            pltpu.make_async_remote_copy(
                buf.at[mine], buf.at[mine], ar_send.at[which], ar_recv.at[which], device_id=to, device_id_type=MESH
            ).start()

    def all_arrived(buf, which):
        n = buf.shape[0]
        pltpu.make_async_copy(buf.at[pl.ds(0, n - 1)], buf.at[pl.ds(0, n - 1)], ar_recv.at[which]).wait()
        s, e = buf[0], jnp.zeros((8, LANE), F32)
        for i in range(1, n):
            s, d = two_sum(s, buf[i])
            e = e + d
        return s + jnp.where(row8 >= 4, pltpu.roll(e, 4, 0), 0.0)

    def all_sent(buf, which):
        n = buf.shape[0]
        pltpu.make_async_copy(buf.at[pl.ds(0, n - 1)], buf.at[pl.ds(0, n - 1)], ar_send.at[which]).wait()

    all_to_one(packed, ar1, mx, [(lax.rem(mx + k, ngx), my, mz) for k in along], 0)

    interpolate_all(handed_q, half, blocks // many)
    loads[5].wait()
    route()
    exchange(tx, rx)
    loads[6].wait()
    pack_halo(prev, sy_i, sz_i, iy, 0)
    prev_halo = send_halo(1, prev, *inner, 0)
    all_to_one(all_arrived(ar1, 0), ar2, my * ngz + mz, [beside(a, b) for a, b in side], 1)
    loads[7].wait()
    loads[8].wait()
    inv[...] = 1.0 / (6.0 + idiag[...])
    v = prev[...]
    p1[...] = source[...] + near_sum(v, iy)
    for c in prev_halo:
        c.wait_recv()
    p1[...] += far_sum(v.shape, hx_i[0], hy_i[0], hz_i[0], at_ends)

    mu_rows = all_arrived(ar2, 1)
    mu = [(mu_rows[k : k + 1], mu_rows[4 + k : 5 + k]) for k in range(4)]
    a0 = mu[0][0] / mu[1][0]
    rr1 = dd_add(mu[0], dd_times(dd_add(dd_times(mu[2], a0), (-2.0 * mu[1][0], -2.0 * mu[1][1])), a0))
    rr1 = rr1[0] + rr1[1]
    beta = rr1 / mu[0][0]
    g = 1.0 + beta
    curve = dd_times(dd_add(dd_times(mu[1], g), dd_times(mu[2], -2.0 * a0)), g)
    curve = dd_add(curve, dd_times(dd_times(mu[3], a0), a0))
    a1 = rr1 / (curve[0] + curve[1])
    c0, c1 = (a0 + a1 * g)[:, :1], (-a0 * a1)[:, :1]
    a0, a1, beta = a0[:, :1], a1[:, :1], beta[:, :1]

    exchanged(rx)
    scatter(c0, c1)
    added = acc[pl.ds(0, ni)] + acc[pl.ds(ni, ni)]
    p1[...] = (p1[...] + added) * inv[...]
    pack_halo(p1, sy_i, sz_i, iy, 1)
    last = send_halo(3, p1, *inner, 1)
    r, q = right[...], q0[...]
    r1 = r - a0 * q
    x_out[...] = a0 * r + a1 * (r1 + beta * r)
    res_out[...] = r1 - a1 * ((q - a0 * q1[...]) + beta * q)
    stores = [
        pltpu.make_async_copy(x_out, x_hbm, store_sem.at[0]),
        pltpu.make_async_copy(res_out, res_hbm, store_sem.at[1]),
    ]
    for c in stores:
        c.start()
    near = source[...] + added + near_sum(p1[...], iy)
    for c in last:
        c.wait_recv()
    p_out[...] = (near + far_sum(near.shape, hx_i[1], hy_i[1], hz_i[1], at_ends)) * inv[...]
    c = pltpu.make_async_copy(p_out, p_hbm, store_sem.at[2])
    c.start()
    stores.append(c)
    for c in first + prev_halo + second + last:
        c.wait_send()
    exchange_sent(tx)
    all_sent(ar1, 0)
    all_sent(ar2, 1)
    for c in stores:
        c.wait()


def solution(mesh):
    ngx, ngy, ngz = (mesh.shape[a] for a in ("gx", "gy", "gz"))
    groups = ngx * ngy

    def per_device(right, odiag, nodes, weights, dest, cell, prev, source, idiag):
        cx, cy, nz = right.shape
        ix, iy, nzi = source.shape
        points = nodes.shape[0]
        cap = 2 * points // groups
        no, ni = cx * cy, ix * iy
        v = pltpu.VMEM
        dma = pltpu.SemaphoreType.DMA
        scratch = [
            v((no, nz), F32), v((no, nz), F32), v((1, points), I32), v((8, points), F32), v((1, points), I32),
            v((1, points), I32), v((ni, nzi), F32), v((ni, nzi), F32), v((ni, nzi), F32), dma((9,)),
            v((no, nz), F32), v((no, nz), F32), v((ni, nzi), F32), v((no, nz), F32), v((no, nz), F32), v((ni, nzi), F32), dma((3,)),
            v((2, 2, cy, nz), F32), v((2, 2, cx, nz), F32), v((2, 2, 8, LANE), F32), v((2, 2, cx, nz), F32), v((2, 2, 8, LANE), F32),
            v((2, 2, iy, nzi), F32), v((2, 2, ix, nzi), F32), v((2, 2, 8, LANE), F32), v((2, 2, ix, nzi), F32), v((2, 2, 8, LANE), F32),
            dma((4, 6)), dma((4, 6)),
            v((ngx, 8, LANE), F32), v((ngy * ngz, 8, LANE), F32), dma((2,)), dma((2,)),
            v((groups, 1, 3 * cap), F32), v((groups, 1, 3 * cap), F32), dma(()), dma(()),
            v((1, points), F32), v((groups, BLK), F32), v((4 * no, nz), BF16), v((1, points), F32), v((1, points), F32),
            v((6 * groups, cap), F32), v((2 * ni, nzi), F32), v((ni, nzi), F32),
        ]
        x, res, p = pl.pallas_call(
            functools.partial(kernel, (ngx, ngy, ngz, cy, iy)),
            out_shape=(
                jax.ShapeDtypeStruct((no, nz), F32),
                jax.ShapeDtypeStruct((no, nz), F32),
                jax.ShapeDtypeStruct((ni, nzi), F32),
            ),
            in_specs=[pl.BlockSpec(memory_space=pl.ANY)] * 9,
            out_specs=[pl.BlockSpec(memory_space=pl.ANY)] * 3,
            scratch_shapes=scratch,
            compiler_params=pltpu.CompilerParams(
                collective_id=0, has_side_effects=True, vmem_limit_bytes=56 * 2**20
            ),
        )(
            right.reshape(no, nz), odiag.reshape(no, nz), nodes.reshape(1, points), weights,
            dest.reshape(1, points), cell.reshape(1, points), prev.reshape(ni, nzi),
            source.reshape(ni, nzi), idiag.reshape(ni, nzi),
        )
        return x.reshape(cx, cy, nz), res.reshape(cx, cy, nz), p.reshape(ix, iy, nzi)

    block = P("gx", "gy", "gz")
    every = ("gx", "gy", "gz")
    return jax.shard_map(
        per_device,
        mesh=mesh,
        in_specs=(block, block, P(every), P(None, every), P(every, None), P(every), block, block, block),
        out_specs=(block, block, block),
        check_vma=False,
    )
```

```python
import functools

import jax
import jax.numpy as jnp
from jax import lax
from jax.experimental import pallas as pl
from jax.experimental.pallas import tpu as pltpu
from jax.sharding import PartitionSpec as P

MESH = pl.DeviceIdType.MESH
F32 = jnp.float32
BF16 = jnp.bfloat16
I32 = jnp.int32
LANE = 128
BLK = 256


def iota(shape, dim):
    return lax.broadcasted_iota(I32, shape, dim)


def halves(x):
    hi = x.astype(BF16).astype(F32)
    return hi, x - hi


def nt(a, b):
    return lax.dot_general(a, b, (((1,), (1,)), ((), ())), preferred_element_type=F32)


def nn(a, b):
    return lax.dot_general(a, b, (((1,), (0,)), ((), ())), preferred_element_type=F32)


def two_sum(a, b):
    s = a + b
    t = s - a
    return s, (a - (s - t)) + (b - t)


def two_prod(a, b):
    p = a * b
    ca, cb = 4097.0 * a, 4097.0 * b
    ah, bh = ca - (ca - a), cb - (cb - b)
    al, bl = a - ah, b - bh
    return p, ((ah * bh - p) + ah * bl + al * bh) + al * bl


def dd_times(x, f):
    p, e = two_prod(x[0], f)
    return two_sum(p, e + x[1] * f)


def dd_add(x, y):
    s, e = two_sum(x[0], y[0])
    return two_sum(s, e + (x[1] + y[1]))


def column(v, at):
    groups = v.shape[0] // 8
    tile = at // LANE * LANE
    lanes = v[:, tile : tile + LANE].reshape(groups, 8, LANE)
    spread = jnp.broadcast_to(lanes[:, :, at - tile : at - tile + 1], (groups, 8, LANE))
    keep = iota((groups, 8, LANE), 2) == iota((groups, 8, LANE), 0)
    return jnp.sum(jnp.where(keep, spread, 0.0), axis=0)


def uncolumn(c, rows):
    groups = rows // 8
    keep = iota((groups, 8, LANE), 2) == iota((groups, 8, LANE), 0)
    picked = jnp.where(keep, jnp.broadcast_to(c[None], (groups, 8, LANE)), 0.0)
    return jnp.sum(picked, axis=2, keepdims=True).reshape(rows, 1)


def near_sum(v, ny):
    rows, nz = v.shape
    zero = jnp.zeros((ny, nz), F32)
    total = jnp.concatenate([zero, v[: rows - ny]], axis=0) + jnp.concatenate([v[ny:], zero], axis=0)
    in_plane = iota((rows, nz), 0) % ny
    lane = iota((rows, nz), 1)
    total = total + jnp.where(in_plane == 0, 0.0, pltpu.roll(v, 1, 0))
    total = total + jnp.where(in_plane == ny - 1, 0.0, pltpu.roll(v, rows - 1, 0))
    total = total + jnp.where(lane == 0, 0.0, pltpu.roll(v, 1, 1))
    return total + jnp.where(lane == nz - 1, 0.0, pltpu.roll(v, nz - 1, 1))


def far_sum(shape, halo_x, halo_y, halo_z, at_ends):
    rows, nz = shape
    ny = halo_x.shape[1]
    planes = rows // ny
    first_x, last_x, first_y, last_y, first_z, last_z = at_ends
    low = jnp.where(first_x, 0.0, halo_x[0])
    high = jnp.where(last_x, 0.0, halo_x[1])
    total = jnp.concatenate([low, jnp.zeros((rows - 2 * ny, nz), F32), high], axis=0)
    in_plane = iota((rows, nz), 0) % ny
    lane = iota((rows, nz), 1)

    def rows_of(h):
        return jnp.broadcast_to(h[:, None, :], (planes, ny, nz)).reshape(rows, nz)

    total = total + jnp.where(in_plane == 0, rows_of(jnp.where(first_y, 0.0, halo_y[0])), 0.0)
    total = total + jnp.where(in_plane == ny - 1, rows_of(jnp.where(last_y, 0.0, halo_y[1])), 0.0)
    total = total + jnp.where(lane == 0, uncolumn(jnp.where(first_z, 0.0, halo_z[0]), rows), 0.0)
    return total + jnp.where(lane == nz - 1, uncolumn(jnp.where(last_z, 0.0, halo_z[1]), rows), 0.0)


def field_of(x):
    nr, nz = x.shape
    ahead = pltpu.roll(x, nz - 1, 1)
    ahead = jnp.where(iota((nr, nz), 1) == nz - 1, pltpu.roll(ahead, nr - 1, 0), ahead)
    hi, lo = halves(jnp.concatenate([x, ahead], axis=0))
    return jnp.concatenate([hi, lo], axis=0).astype(BF16)


def hot_bf16(ids, wanted, value):
    return jnp.where(ids == wanted.astype(BF16), jnp.broadcast_to(value.astype(BF16), ids.shape), jnp.zeros(ids.shape, BF16))


def interpolate(field, n, w, cy, nz):
    nr = field.shape[0] // 4
    planes, parts, blk = nr // cy, cy // 8, n.shape[1]
    row = n // nz
    a0 = jnp.broadcast_to(row // cy, (8, blk))
    b0 = jnp.broadcast_to(row % cy, (8, blk))
    column_hot = hot_bf16(iota((nz, blk), 0).astype(BF16), n % nz, jnp.ones((1, blk), F32))
    got = nn(field, column_hot)
    got = got[: 2 * nr] + got[2 * nr :]
    here = [a0 == a for a in range(planes - 1)]

    def pick(dc, part, ahead):
        def at(a):
            s = dc * nr + min(a + ahead, planes - 1) * cy + part * 8
            return got[s : s + 8]

        v = at(planes - 2)
        for a in range(planes - 3, -1, -1):
            v = jnp.where(here[a], at(a), v)
        return v

    sub = iota((8, blk), 0)
    total = jnp.zeros((8, blk), F32)
    for dc in range(2):
        picked = [[pick(dc, part, ahead) for part in range(parts)] for ahead in range(2)] + [[pick(dc, 0, 2)]]
        for da in range(2):
            wa, wb = w(da * 4 + dc), w(da * 4 + 2 + dc)
            for part in range(parts):
                wt = jnp.where(b0 == sub + 8 * part, wa, jnp.where(b0 + 1 == sub + 8 * part, wb, 0.0))
                total = total + wt * picked[da][part]
            total = total + jnp.where(b0 + 1 == sub + cy, wb, 0.0) * picked[da + 1][0]
    return jnp.sum(total, axis=0, keepdims=True)


def kernel(
    sizes,
    right_hbm, odiag_hbm, nodes_hbm, weights_hbm, dest_hbm, cell_hbm, prev_hbm, source_hbm, idiag_hbm,
    x_hbm, res_hbm, p_hbm,
    right, odiag, nodes, weights, dest, cell, prev, source, idiag, load_sem,
    q0, q1, p1, x_out, res_out, p_out, store_sem,
    hx_o, hy_o, hz_o, sy_o, sz_o, hx_i, hy_i, hz_i, sy_i, sz_i, halo_send, halo_recv,
    ar1, ar2, ar_send, ar_recv,
    tx, rx, a2a_send, a2a_recv, ready,
    rank, carry, field, handed_r, handed_q, routed, acc, inv,
):
    ngx, ngy, ngz, cy, iy = sizes
    mx, my, mz = lax.axis_index("gx"), lax.axis_index("gy"), lax.axis_index("gz")
    groups = ngx * ngy
    me = mx * ngy + my
    points = nodes.shape[1]
    blocks = points // BLK
    cap = tx.shape[2] // 3
    at_ends = (mx == 0, mx == ngx - 1, my == 0, my == ngy - 1, mz == 0, mz == ngz - 1)

    barrier = pltpu.get_barrier_semaphore()

    def peer(k):
        t = lax.rem(me + k, groups)
        return t, (t // ngy, lax.rem(t, ngy), mz)

    loads = []
    for i, (a, b) in enumerate(
        ((right_hbm, right), (dest_hbm, dest), (nodes_hbm, nodes), (weights_hbm, weights), (odiag_hbm, odiag),
         (cell_hbm, cell), (prev_hbm, prev), (source_hbm, source), (idiag_hbm, idiag))
    ):
        c = pltpu.make_async_copy(a, b, load_sem.at[i])
        c.start()
        loads.append(c)
    side = [(a, b) for a in range(ngy) for b in range(ngz) if (a, b) != (0, 0)]
    side.sort(key=lambda t: -(min(t[0], ngy - t[0]) + min(t[1], ngz - t[1])))
    along = sorted(range(1, ngx), key=lambda k: -min(k, ngx - k))

    def beside(a, b):
        return (mx, lax.rem(my + a, ngy), lax.rem(mz + b, ngz))

    line = [(lax.rem(mx + k, ngx), my, mz) for k in along]
    layer = [beside(a, b) for a, b in side]
    for to in line + layer:
        pl.semaphore_signal(barrier, inc=1, device_id=to, device_id_type=MESH)

    up = ((lax.rem(mx + 1, ngx), my, mz), (mx, lax.rem(my + 1, ngy), mz), (mx, my, lax.rem(mz + 1, ngz)))
    down = (
        (lax.rem(mx + ngx - 1, ngx), my, mz),
        (mx, lax.rem(my + ngy - 1, ngy), mz),
        (mx, my, lax.rem(mz + ngz - 1, ngz)),
    )

    def pack_halo(src, sy, sz, ny, slot):
        rows, nz = src.shape
        v = src[...]
        solid = v.reshape(rows // ny, ny, nz)
        sy[slot, 0] = solid[:, ny - 1, :]
        sy[slot, 1] = solid[:, 0, :]
        sz[slot, 0] = column(v, nz - 1)
        sz[slot, 1] = column(v, 0)

    def send_halo(which, src, hx, hy, hz, sy, sz, slot):
        rows = src.shape[0]
        ny = hx.shape[2]
        copies = []

        def send(j, a, b, to):
            c = pltpu.make_async_remote_copy(
                a, b, halo_send.at[which, j], halo_recv.at[which, j], device_id=to, device_id_type=MESH
            )
            c.start()
            copies.append(c)

        send(0, src.at[pl.ds(rows - ny, ny)], hx.at[slot, 0], up[0])
        send(1, src.at[pl.ds(0, ny)], hx.at[slot, 1], down[0])
        send(2, sy.at[slot, 0], hy.at[slot, 0], up[1])
        send(3, sy.at[slot, 1], hy.at[slot, 1], down[1])
        send(4, sz.at[slot, 0], hz.at[slot, 0], up[2])
        send(5, sz.at[slot, 1], hz.at[slot, 1], down[2])
        return copies

    outer = (hx_o, hy_o, hz_o, sy_o, sz_o)
    inner = (hx_i, hy_i, hz_i, sy_i, sz_i)
    nz = right.shape[1]

    def rank_points():
        low = iota((BLK, BLK), 0) < iota((BLK, BLK), 1)
        tri = jnp.concatenate([jnp.where(low, 1.0, 0.0), jnp.ones((BLK, BLK), F32)], axis=1).astype(BF16)
        carry[...] = jnp.zeros_like(carry)
        step = next(s for s in (16, 4, 1) if blocks % s == 0)
        ids = iota((groups, BLK), 0)
        one = jnp.ones((1, BLK), F32)

        def rank_step(j, _):
            seen = carry[...]
            for b in range(step):
                at = pl.ds(pl.multiple_of((j * step + b) * BLK, BLK), BLK)
                name = dest[:, at]
                part = nn(hot_bf16(ids.astype(BF16), name, one), tri)
                rank[:, at] = jnp.sum(jnp.where(ids == name, part[:, :BLK] + seen, 0.0), axis=0, keepdims=True)
                seen = seen + part[:, BLK:]
            carry[...] = seen
            return 0

        lax.fori_loop(0, blocks // step, rank_step, 0)

    many = next(s for s in (16, 4, 1) if blocks % s == 0)

    def interpolate_all(handed, first, end):
        def go(j, _):
            for b in range(many):
                at = pl.ds(pl.multiple_of((j * many + b) * BLK, BLK), BLK)
                handed[:, at] = interpolate(field[...], nodes[:, at], lambda k: weights[k : k + 1, at], cy, nz)
            return 0

        lax.fori_loop(first, end, go, 0)

    def route():
        ids = iota((groups, BLK), 0).astype(BF16)
        slots = iota((cap, BLK), 0).astype(BF16)
        one = jnp.ones((1, BLK), F32)
        routed[...] = jnp.zeros_like(routed)

        def go(j, _):
            part = jnp.zeros(routed.shape, F32)
            for b in range(many):
                at = pl.ds(pl.multiple_of((j * many + b) * BLK, BLK), BLK)
                c = cell[:, at]
                values = (*halves(handed_r[:, at]), *halves(handed_q[:, at]), (c // 256).astype(F32), (c % 256).astype(F32))
                left = jnp.concatenate([hot_bf16(ids, dest[:, at], v) for v in values], axis=0)
                part = part + nt(left, hot_bf16(slots, rank[:, at], one))
            routed[...] += part
            return 0

        lax.fori_loop(0, blocks // many, go, 0)
        rows = [routed[pl.ds(i * groups, groups)] for i in range(6)]
        tx[...] = jnp.concatenate([rows[0] + rows[1], rows[2] + rows[3], rows[4] * 256.0 + rows[5]], axis=1).reshape(
            groups, 1, 3 * cap
        )

    middle = groups // 2

    def exchange(src, dst):
        def go(i, _):
            half = (i + 1) // 2
            t, to = peer(middle + jnp.where(lax.rem(i, 2) == 1, half, -half))
            pltpu.make_async_remote_copy(
                src.at[t], dst.at[me], a2a_send, a2a_recv, device_id=to, device_id_type=MESH
            ).start()
            return 0

        lax.fori_loop(0, groups - 1, go, 0)
        dst[pl.ds(me, 1)] = src[pl.ds(me, 1)]

    def exchanged(dst):
        all_but_one = pl.ds(0, groups - 1)
        pltpu.make_async_copy(dst.at[all_but_one], dst.at[all_but_one], a2a_recv).wait()

    def exchange_sent(src):
        all_but_one = pl.ds(0, groups - 1)
        pltpu.make_async_copy(src.at[all_but_one], src.at[all_but_one], a2a_send).wait()

    batch = next(s for s in (16, 8, 4, 2, 1) if groups % s == 0)
    ni, nzi = source.shape

    def scatter(c0, c1):
        rows_id = iota((ni, cap), 0).astype(BF16)
        cols_id = iota((nzi, cap), 0).astype(BF16)
        one = jnp.ones((1, cap), F32)
        acc[...] = jnp.zeros_like(acc)

        def go(j, _):
            part = jnp.zeros(acc.shape, F32)
            for b in range(batch):
                got = rx[j * batch + b]
                c = got[:, 2 * cap :].astype(I32)
                hi, lo = halves(c0 * got[:, :cap] + c1 * got[:, cap : 2 * cap])
                left = jnp.concatenate([hot_bf16(rows_id, c // nzi, hi), hot_bf16(rows_id, c // nzi, lo)], axis=0)
                part = part + nt(left, hot_bf16(cols_id, c % nzi, one))
            acc[...] += part
            return 0

        lax.fori_loop(0, groups // batch, go, 0)

    loads[0].wait()
    pack_halo(right, sy_o, sz_o, cy, 0)
    pl.semaphore_wait(barrier, len(line) + len(layer))
    first = send_halo(0, right, *outer, 0)
    for to in line:
        pl.semaphore_signal(ready, inc=1, device_id=to, device_id_type=MESH)
    field[...] = field_of(right[...])
    loads[2].wait()
    loads[3].wait()
    interpolate_all(handed_r, 0, blocks // many)
    loads[1].wait()
    rank_points()

    loads[4].wait()
    r = right[...]
    near = (6.0 + odiag[...]) * r - near_sum(r, cy)
    for c in first:
        c.wait_recv()
    q0[...] = near - far_sum(r.shape, hx_o[0], hy_o[0], hz_o[0], at_ends)
    pack_halo(q0, sy_o, sz_o, cy, 1)
    second = send_halo(2, q0, *outer, 1)
    field[...] = field_of(q0[...])
    interpolate_all(handed_q, 0, blocks // many)

    q = q0[...]
    near = (6.0 + odiag[...]) * q - near_sum(q, cy)
    for c in second:
        c.wait_recv()
    q1[...] = near - far_sum(q.shape, hx_o[1], hy_o[1], hz_o[1], at_ends)
    row8 = iota((8, LANE), 0)
    packed = jnp.zeros((8, LANE), F32)
    r, qq = right[...], q1[...]
    for k, (a, b) in enumerate(((r, r), (r, q), (q, q), (q, qq))):
        s = jnp.sum((a * b).reshape(-1, 8, nz), axis=0)
        t = s[:, :LANE]
        for m in range(LANE, nz, LANE):
            t = t + s[:, m : m + LANE]
        packed = jnp.where(row8 == k, jnp.sum(t, axis=0, keepdims=True), packed)
    packed = jnp.broadcast_to(jnp.sum(packed, axis=1, keepdims=True), (8, LANE))

    def all_to_one(value, buf, mine, partners, which):
        buf[pl.ds(mine, 1)] = value[None]
        for to in partners:
            pltpu.make_async_remote_copy(
                buf.at[mine], buf.at[mine], ar_send.at[which], ar_recv.at[which], device_id=to, device_id_type=MESH
            ).start()

    def all_arrived(buf, which):
        n = buf.shape[0]
        pltpu.make_async_copy(buf.at[pl.ds(0, n - 1)], buf.at[pl.ds(0, n - 1)], ar_recv.at[which]).wait()
        s, e = buf[0], jnp.zeros((8, LANE), F32)
        for i in range(1, n):
            s, d = two_sum(s, buf[i])
            e = e + d
        return s + jnp.where(row8 >= 4, pltpu.roll(e, 4, 0), 0.0)

    def all_sent(buf, which):
        n = buf.shape[0]
        pltpu.make_async_copy(buf.at[pl.ds(0, n - 1)], buf.at[pl.ds(0, n - 1)], ar_send.at[which]).wait()

    all_to_one(packed, ar1, mx, line, 0)

    loads[5].wait()
    route()
    pl.semaphore_wait(ready, len(line))
    exchange(tx, rx)
    loads[6].wait()
    pack_halo(prev, sy_i, sz_i, iy, 0)
    prev_halo = send_halo(1, prev, *inner, 0)
    all_to_one(all_arrived(ar1, 0), ar2, my * ngz + mz, layer, 1)
    loads[7].wait()
    loads[8].wait()
    inv[...] = 1.0 / (6.0 + idiag[...])
    v = prev[...]
    p1[...] = source[...] + near_sum(v, iy)
    for c in prev_halo:
        c.wait_recv()
    p1[...] += far_sum(v.shape, hx_i[0], hy_i[0], hz_i[0], at_ends)

    mu_rows = all_arrived(ar2, 1)
    mu = [(mu_rows[k : k + 1], mu_rows[4 + k : 5 + k]) for k in range(4)]
    a0 = mu[0][0] / mu[1][0]
    rr1 = dd_add(mu[0], dd_times(dd_add(dd_times(mu[2], a0), (-2.0 * mu[1][0], -2.0 * mu[1][1])), a0))
    rr1 = rr1[0] + rr1[1]
    beta = rr1 / mu[0][0]
    g = 1.0 + beta
    curve = dd_times(dd_add(dd_times(mu[1], g), dd_times(mu[2], -2.0 * a0)), g)
    curve = dd_add(curve, dd_times(dd_times(mu[3], a0), a0))
    a1 = rr1 / (curve[0] + curve[1])
    c0, c1 = (a0 + a1 * g)[:, :1], (-a0 * a1)[:, :1]
    a0, a1, beta = a0[:, :1], a1[:, :1], beta[:, :1]

    exchanged(rx)
    scatter(c0, c1)
    added = acc[pl.ds(0, ni)] + acc[pl.ds(ni, ni)]
    p1[...] = (p1[...] + added) * inv[...]
    pack_halo(p1, sy_i, sz_i, iy, 1)
    last = send_halo(3, p1, *inner, 1)
    r, q = right[...], q0[...]
    r1 = r - a0 * q
    x_out[...] = a0 * r + a1 * (r1 + beta * r)
    res_out[...] = r1 - a1 * ((q - a0 * q1[...]) + beta * q)
    stores = [
        pltpu.make_async_copy(x_out, x_hbm, store_sem.at[0]),
        pltpu.make_async_copy(res_out, res_hbm, store_sem.at[1]),
    ]
    for c in stores:
        c.start()
    near = source[...] + added + near_sum(p1[...], iy)
    for c in last:
        c.wait_recv()
    p_out[...] = (near + far_sum(near.shape, hx_i[1], hy_i[1], hz_i[1], at_ends)) * inv[...]
    c = pltpu.make_async_copy(p_out, p_hbm, store_sem.at[2])
    c.start()
    stores.append(c)
    for c in first + prev_halo + second + last:
        c.wait_send()
    exchange_sent(tx)
    all_sent(ar1, 0)
    all_sent(ar2, 1)
    for c in stores:
        c.wait()


def solution(mesh):
    ngx, ngy, ngz = (mesh.shape[a] for a in ("gx", "gy", "gz"))
    groups = ngx * ngy

    def per_device(right, odiag, nodes, weights, dest, cell, prev, source, idiag):
        cx, cy, nz = right.shape
        ix, iy, nzi = source.shape
        points = nodes.shape[0]
        cap = 2 * points // groups
        no, ni = cx * cy, ix * iy
        v = pltpu.VMEM
        dma = pltpu.SemaphoreType.DMA
        scratch = [
            v((no, nz), F32), v((no, nz), F32), v((1, points), I32), v((8, points), F32), v((1, points), I32),
            v((1, points), I32), v((ni, nzi), F32), v((ni, nzi), F32), v((ni, nzi), F32), dma((9,)),
            v((no, nz), F32), v((no, nz), F32), v((ni, nzi), F32), v((no, nz), F32), v((no, nz), F32), v((ni, nzi), F32), dma((3,)),
            v((2, 2, cy, nz), F32), v((2, 2, cx, nz), F32), v((2, 2, 8, LANE), F32), v((2, 2, cx, nz), F32), v((2, 2, 8, LANE), F32),
            v((2, 2, iy, nzi), F32), v((2, 2, ix, nzi), F32), v((2, 2, 8, LANE), F32), v((2, 2, ix, nzi), F32), v((2, 2, 8, LANE), F32),
            dma((4, 6)), dma((4, 6)),
            v((ngx, 8, LANE), F32), v((ngy * ngz, 8, LANE), F32), dma((2,)), dma((2,)),
            v((groups, 1, 3 * cap), F32), v((groups, 1, 3 * cap), F32), dma(()), dma(()), pltpu.SemaphoreType.REGULAR,
            v((1, points), F32), v((groups, BLK), F32), v((4 * no, nz), BF16), v((1, points), F32), v((1, points), F32),
            v((6 * groups, cap), F32), v((2 * ni, nzi), F32), v((ni, nzi), F32),
        ]
        x, res, p = pl.pallas_call(
            functools.partial(kernel, (ngx, ngy, ngz, cy, iy)),
            out_shape=(
                jax.ShapeDtypeStruct((no, nz), F32),
                jax.ShapeDtypeStruct((no, nz), F32),
                jax.ShapeDtypeStruct((ni, nzi), F32),
            ),
            in_specs=[pl.BlockSpec(memory_space=pl.ANY)] * 9,
            out_specs=[pl.BlockSpec(memory_space=pl.ANY)] * 3,
            scratch_shapes=scratch,
            compiler_params=pltpu.CompilerParams(
                collective_id=0, has_side_effects=True, vmem_limit_bytes=56 * 2**20
            ),
        )(
            right.reshape(no, nz), odiag.reshape(no, nz), nodes.reshape(1, points), weights,
            dest.reshape(1, points), cell.reshape(1, points), prev.reshape(ni, nzi),
            source.reshape(ni, nzi), idiag.reshape(ni, nzi),
        )
        return x.reshape(cx, cy, nz), res.reshape(cx, cy, nz), p.reshape(ix, iy, nzi)

    block = P("gx", "gy", "gz")
    every = ("gx", "gy", "gz")
    return jax.shard_map(
        per_device,
        mesh=mesh,
        in_specs=(block, block, P(every), P(None, every), P(every, None), P(every), block, block, block),
        out_specs=(block, block, block),
        check_vma=False,
    )
```

```python
import functools

import jax
import jax.numpy as jnp
from jax import lax
from jax.experimental import pallas as pl
from jax.experimental.pallas import tpu as pltpu
from jax.sharding import PartitionSpec as P

MESH = pl.DeviceIdType.MESH
F32 = jnp.float32
BF16 = jnp.bfloat16
I32 = jnp.int32
LANE = 128
BLK = 256


def iota(shape, dim):
    return lax.broadcasted_iota(I32, shape, dim)


def halves(x):
    hi = x.astype(BF16).astype(F32)
    return hi, x - hi


def nt(a, b):
    return lax.dot_general(a, b, (((1,), (1,)), ((), ())), preferred_element_type=F32)


def nn(a, b):
    return lax.dot_general(a, b, (((1,), (0,)), ((), ())), preferred_element_type=F32)


def two_sum(a, b):
    s = a + b
    t = s - a
    return s, (a - (s - t)) + (b - t)


def two_prod(a, b):
    p = a * b
    ca, cb = 4097.0 * a, 4097.0 * b
    ah, bh = ca - (ca - a), cb - (cb - b)
    al, bl = a - ah, b - bh
    return p, ((ah * bh - p) + ah * bl + al * bh) + al * bl


def dd_times(x, f):
    p, e = two_prod(x[0], f)
    return two_sum(p, e + x[1] * f)


def dd_add(x, y):
    s, e = two_sum(x[0], y[0])
    return two_sum(s, e + (x[1] + y[1]))


def column(v, at):
    groups = v.shape[0] // 8
    tile = at // LANE * LANE
    lanes = v[:, tile : tile + LANE].reshape(groups, 8, LANE)
    spread = jnp.broadcast_to(lanes[:, :, at - tile : at - tile + 1], (groups, 8, LANE))
    keep = iota((groups, 8, LANE), 2) == iota((groups, 8, LANE), 0)
    return jnp.sum(jnp.where(keep, spread, 0.0), axis=0)


def uncolumn(c, rows):
    groups = rows // 8
    keep = iota((groups, 8, LANE), 2) == iota((groups, 8, LANE), 0)
    picked = jnp.where(keep, jnp.broadcast_to(c[None], (groups, 8, LANE)), 0.0)
    return jnp.sum(picked, axis=2, keepdims=True).reshape(rows, 1)


def near_sum(v, ny):
    rows, nz = v.shape
    zero = jnp.zeros((ny, nz), F32)
    total = jnp.concatenate([zero, v[: rows - ny]], axis=0) + jnp.concatenate([v[ny:], zero], axis=0)
    in_plane = iota((rows, nz), 0) % ny
    lane = iota((rows, nz), 1)
    total = total + jnp.where(in_plane == 0, 0.0, pltpu.roll(v, 1, 0))
    total = total + jnp.where(in_plane == ny - 1, 0.0, pltpu.roll(v, rows - 1, 0))
    total = total + jnp.where(lane == 0, 0.0, pltpu.roll(v, 1, 1))
    return total + jnp.where(lane == nz - 1, 0.0, pltpu.roll(v, nz - 1, 1))


def far_sum(shape, halo_x, halo_y, halo_z, at_ends):
    rows, nz = shape
    ny = halo_x.shape[1]
    planes = rows // ny
    first_x, last_x, first_y, last_y, first_z, last_z = at_ends
    low = jnp.where(first_x, 0.0, halo_x[0])
    high = jnp.where(last_x, 0.0, halo_x[1])
    total = jnp.concatenate([low, jnp.zeros((rows - 2 * ny, nz), F32), high], axis=0)
    in_plane = iota((rows, nz), 0) % ny
    lane = iota((rows, nz), 1)

    def rows_of(h):
        return jnp.broadcast_to(h[:, None, :], (planes, ny, nz)).reshape(rows, nz)

    total = total + jnp.where(in_plane == 0, rows_of(jnp.where(first_y, 0.0, halo_y[0])), 0.0)
    total = total + jnp.where(in_plane == ny - 1, rows_of(jnp.where(last_y, 0.0, halo_y[1])), 0.0)
    total = total + jnp.where(lane == 0, uncolumn(jnp.where(first_z, 0.0, halo_z[0]), rows), 0.0)
    return total + jnp.where(lane == nz - 1, uncolumn(jnp.where(last_z, 0.0, halo_z[1]), rows), 0.0)


def field_of(x):
    nr, nz = x.shape
    ahead = pltpu.roll(x, nz - 1, 1)
    ahead = jnp.where(iota((nr, nz), 1) == nz - 1, pltpu.roll(ahead, nr - 1, 0), ahead)
    hi, lo = halves(jnp.concatenate([x, ahead], axis=0))
    return jnp.concatenate([hi, lo], axis=0).astype(BF16)


def hot_bf16(ids, wanted, value):
    return jnp.where(ids == wanted.astype(BF16), jnp.broadcast_to(value.astype(BF16), ids.shape), jnp.zeros(ids.shape, BF16))


def interpolate(field, n, w, cy, nz):
    nr = field.shape[0] // 4
    planes, parts, blk = nr // cy, cy // 8, n.shape[1]
    row = n // nz
    a0 = jnp.broadcast_to(row // cy, (8, blk))
    b0 = jnp.broadcast_to(row % cy, (8, blk))
    column_hot = hot_bf16(iota((nz, blk), 0).astype(BF16), n % nz, jnp.ones((1, blk), F32))
    got = nn(field, column_hot)
    got = got[: 2 * nr] + got[2 * nr :]
    here = [a0 == a for a in range(planes - 1)]

    def pick(dc, part, ahead):
        def at(a):
            s = dc * nr + min(a + ahead, planes - 1) * cy + part * 8
            return got[s : s + 8]

        v = at(planes - 2)
        for a in range(planes - 3, -1, -1):
            v = jnp.where(here[a], at(a), v)
        return v

    sub = iota((8, blk), 0)
    total = jnp.zeros((8, blk), F32)
    for dc in range(2):
        picked = [[pick(dc, part, ahead) for part in range(parts)] for ahead in range(2)] + [[pick(dc, 0, 2)]]
        for da in range(2):
            wa, wb = w(da * 4 + dc), w(da * 4 + 2 + dc)
            for part in range(parts):
                wt = jnp.where(b0 == sub + 8 * part, wa, jnp.where(b0 + 1 == sub + 8 * part, wb, 0.0))
                total = total + wt * picked[da][part]
            total = total + jnp.where(b0 + 1 == sub + cy, wb, 0.0) * picked[da + 1][0]
    return jnp.sum(total, axis=0, keepdims=True)


def kernel(
    sizes,
    right_hbm, odiag_hbm, nodes_hbm, weights_hbm, dest_hbm, cell_hbm, prev_hbm, source_hbm, idiag_hbm,
    x_hbm, res_hbm, p_hbm,
    right, odiag, nodes, weights, dest, cell, prev, source, idiag, load_sem,
    q0, q1, p1, x_out, res_out, p_out, store_sem,
    hx_o, hy_o, hz_o, sy_o, sz_o, hx_i, hy_i, hz_i, sy_i, sz_i, halo_send, halo_recv,
    ar1, ar2, ar_send, ar_recv,
    tx, rx, a2a_send, a2a_recv, ready,
    rank, carry, field, handed_r, handed_q, routed, acc, inv,
):
    ngx, ngy, ngz, cy, iy = sizes
    mx, my, mz = lax.axis_index("gx"), lax.axis_index("gy"), lax.axis_index("gz")
    groups = ngx * ngy
    me = mx * ngy + my
    points = nodes.shape[1]
    blocks = points // BLK
    cap = tx.shape[2] // 3
    at_ends = (mx == 0, mx == ngx - 1, my == 0, my == ngy - 1, mz == 0, mz == ngz - 1)

    barrier = pltpu.get_barrier_semaphore()

    def peer(k):
        t = lax.rem(me + k, groups)
        return t, (t // ngy, lax.rem(t, ngy), mz)

    loads = []
    for i, (a, b) in enumerate(
        ((right_hbm, right), (dest_hbm, dest), (nodes_hbm, nodes), (weights_hbm, weights), (odiag_hbm, odiag),
         (cell_hbm, cell), (prev_hbm, prev), (source_hbm, source), (idiag_hbm, idiag))
    ):
        c = pltpu.make_async_copy(a, b, load_sem.at[i])
        c.start()
        loads.append(c)
    side = [(a, b) for a in range(ngy) for b in range(ngz) if (a, b) != (0, 0)]
    side.sort(key=lambda t: -(min(t[0], ngy - t[0]) + min(t[1], ngz - t[1])))
    along = sorted(range(1, ngx), key=lambda k: -min(k, ngx - k))

    def beside(a, b):
        return (mx, lax.rem(my + a, ngy), lax.rem(mz + b, ngz))

    line = [(lax.rem(mx + k, ngx), my, mz) for k in along]
    layer = [beside(a, b) for a, b in side]
    for to in line + layer:
        pl.semaphore_signal(barrier, inc=1, device_id=to, device_id_type=MESH)

    up = ((lax.rem(mx + 1, ngx), my, mz), (mx, lax.rem(my + 1, ngy), mz), (mx, my, lax.rem(mz + 1, ngz)))
    down = (
        (lax.rem(mx + ngx - 1, ngx), my, mz),
        (mx, lax.rem(my + ngy - 1, ngy), mz),
        (mx, my, lax.rem(mz + ngz - 1, ngz)),
    )

    def pack_halo(src, sy, sz, ny, slot):
        rows, nz = src.shape
        v = src[...]
        solid = v.reshape(rows // ny, ny, nz)
        sy[slot, 0] = solid[:, ny - 1, :]
        sy[slot, 1] = solid[:, 0, :]
        sz[slot, 0] = column(v, nz - 1)
        sz[slot, 1] = column(v, 0)

    def send_halo(which, src, hx, hy, hz, sy, sz, slot):
        rows = src.shape[0]
        ny = hx.shape[2]
        copies = []

        def send(j, a, b, to):
            c = pltpu.make_async_remote_copy(
                a, b, halo_send.at[which, j], halo_recv.at[which, j], device_id=to, device_id_type=MESH
            )
            c.start()
            copies.append(c)

        send(0, src.at[pl.ds(rows - ny, ny)], hx.at[slot, 0], up[0])
        send(1, src.at[pl.ds(0, ny)], hx.at[slot, 1], down[0])
        send(2, sy.at[slot, 0], hy.at[slot, 0], up[1])
        send(3, sy.at[slot, 1], hy.at[slot, 1], down[1])
        send(4, sz.at[slot, 0], hz.at[slot, 0], up[2])
        send(5, sz.at[slot, 1], hz.at[slot, 1], down[2])
        return copies

    outer = (hx_o, hy_o, hz_o, sy_o, sz_o)
    inner = (hx_i, hy_i, hz_i, sy_i, sz_i)
    nz = right.shape[1]

    def rank_points():
        low = iota((BLK, BLK), 0) < iota((BLK, BLK), 1)
        tri = jnp.concatenate([jnp.where(low, 1.0, 0.0), jnp.ones((BLK, BLK), F32)], axis=1).astype(BF16)
        carry[...] = jnp.zeros_like(carry)
        step = next(s for s in (16, 4, 1) if blocks % s == 0)
        ids = iota((groups, BLK), 0)
        one = jnp.ones((1, BLK), F32)

        def rank_step(j, _):
            seen = carry[...]
            for b in range(step):
                at = pl.ds(pl.multiple_of((j * step + b) * BLK, BLK), BLK)
                name = dest[:, at]
                part = nn(hot_bf16(ids.astype(BF16), name, one), tri)
                rank[:, at] = jnp.sum(jnp.where(ids == name, part[:, :BLK] + seen, 0.0), axis=0, keepdims=True)
                seen = seen + part[:, BLK:]
            carry[...] = seen
            return 0

        lax.fori_loop(0, blocks // step, rank_step, 0)

    many = next(s for s in (16, 4, 1) if blocks % s == 0)

    def interpolate_all(handed, first, end):
        def go(j, _):
            for b in range(many):
                at = pl.ds(pl.multiple_of((j * many + b) * BLK, BLK), BLK)
                handed[:, at] = interpolate(field[...], nodes[:, at], lambda k: weights[k : k + 1, at], cy, nz)
            return 0

        lax.fori_loop(first, end, go, 0)

    def route():
        ids = iota((groups, BLK), 0).astype(BF16)
        slots = iota((cap, BLK), 0).astype(BF16)
        one = jnp.ones((1, BLK), F32)
        routed[...] = jnp.zeros_like(routed)

        def go(j, _):
            part = jnp.zeros(routed.shape, F32)
            for b in range(many):
                at = pl.ds(pl.multiple_of((j * many + b) * BLK, BLK), BLK)
                c = cell[:, at]
                values = (*halves(handed_r[:, at]), *halves(handed_q[:, at]), (c // 256).astype(F32), (c % 256).astype(F32))
                left = jnp.concatenate([hot_bf16(ids, dest[:, at], v) for v in values], axis=0)
                part = part + nt(left, hot_bf16(slots, rank[:, at], one))
            routed[...] += part
            return 0

        lax.fori_loop(0, blocks // many, go, 0)
        rows = [routed[pl.ds(i * groups, groups)] for i in range(6)]
        tx[...] = jnp.concatenate([rows[0] + rows[1], rows[2] + rows[3], rows[4] * 256.0 + rows[5]], axis=1).reshape(
            groups, 1, 3 * cap
        )

    middle = groups // 2
    batch = next(s for s in (16, 8, 4, 2, 1) if groups % s == 0)

    def offset(i):
        half = (i + 1) // 2
        return middle + jnp.where(lax.rem(i, 2) == 1, half, -half)

    def exchange(src, dst):
        def go(i, _):
            t, to = peer(offset(i))
            pltpu.make_async_remote_copy(
                src.at[t], dst.at[me], a2a_send, a2a_recv.at[i // batch], device_id=to, device_id_type=MESH
            ).start()
            return 0

        lax.fori_loop(0, groups - 1, go, 0)
        pltpu.make_async_copy(src.at[me], dst.at[me], a2a_recv.at[groups // batch - 1]).start()

    def exchanged(dst, j):
        pltpu.make_async_copy(dst.at[pl.ds(0, batch)], dst.at[pl.ds(0, batch)], a2a_recv.at[j]).wait()

    def exchange_sent(src):
        all_but_one = pl.ds(0, groups - 1)
        pltpu.make_async_copy(src.at[all_but_one], src.at[all_but_one], a2a_send).wait()

    ni, nzi = source.shape

    def scatter(c0, c1):
        rows_id = iota((ni, cap), 0).astype(BF16)
        cols_id = iota((nzi, cap), 0).astype(BF16)
        one = jnp.ones((1, cap), F32)
        acc[...] = jnp.zeros_like(acc)

        def go(j, _):
            exchanged(rx, j)
            part = jnp.zeros(acc.shape, F32)
            for b in range(batch):
                got = rx[lax.rem(me + 2 * groups - offset(j * batch + b), groups)]
                c = got[:, 2 * cap :].astype(I32)
                hi, lo = halves(c0 * got[:, :cap] + c1 * got[:, cap : 2 * cap])
                left = jnp.concatenate([hot_bf16(rows_id, c // nzi, hi), hot_bf16(rows_id, c // nzi, lo)], axis=0)
                part = part + nt(left, hot_bf16(cols_id, c % nzi, one))
            acc[...] += part
            return 0

        lax.fori_loop(0, groups // batch, go, 0)

    loads[0].wait()
    pack_halo(right, sy_o, sz_o, cy, 0)
    field[...] = field_of(right[...])
    loads[1].wait()
    rank_points()
    pl.semaphore_wait(barrier, len(line) + len(layer))
    first = send_halo(0, right, *outer, 0)
    for to in line:
        pl.semaphore_signal(ready, inc=1, device_id=to, device_id_type=MESH)
    loads[2].wait()
    loads[3].wait()
    interpolate_all(handed_r, 0, blocks // many)

    loads[4].wait()
    r = right[...]
    near = (6.0 + odiag[...]) * r - near_sum(r, cy)
    for c in first:
        c.wait_recv()
    q0[...] = near - far_sum(r.shape, hx_o[0], hy_o[0], hz_o[0], at_ends)
    pack_halo(q0, sy_o, sz_o, cy, 1)
    second = send_halo(2, q0, *outer, 1)
    field[...] = field_of(q0[...])
    interpolate_all(handed_q, 0, blocks // many)

    q = q0[...]
    near = (6.0 + odiag[...]) * q - near_sum(q, cy)
    for c in second:
        c.wait_recv()
    q1[...] = near - far_sum(q.shape, hx_o[1], hy_o[1], hz_o[1], at_ends)
    row8 = iota((8, LANE), 0)
    packed = jnp.zeros((8, LANE), F32)
    r, qq = right[...], q1[...]
    for k, (a, b) in enumerate(((r, r), (r, q), (q, q), (q, qq))):
        s = jnp.sum((a * b).reshape(-1, 8, nz), axis=0)
        t = s[:, :LANE]
        for m in range(LANE, nz, LANE):
            t = t + s[:, m : m + LANE]
        packed = jnp.where(row8 == k, jnp.sum(t, axis=0, keepdims=True), packed)
    packed = jnp.broadcast_to(jnp.sum(packed, axis=1, keepdims=True), (8, LANE))

    def all_to_one(value, buf, mine, partners, which):
        buf[pl.ds(mine, 1)] = value[None]
        for to in partners:
            pltpu.make_async_remote_copy(
                buf.at[mine], buf.at[mine], ar_send.at[which], ar_recv.at[which], device_id=to, device_id_type=MESH
            ).start()

    def all_arrived(buf, which):
        n = buf.shape[0]
        pltpu.make_async_copy(buf.at[pl.ds(0, n - 1)], buf.at[pl.ds(0, n - 1)], ar_recv.at[which]).wait()
        s, e = buf[0], jnp.zeros((8, LANE), F32)
        for i in range(1, n):
            s, d = two_sum(s, buf[i])
            e = e + d
        return s + jnp.where(row8 >= 4, pltpu.roll(e, 4, 0), 0.0)

    def all_sent(buf, which):
        n = buf.shape[0]
        pltpu.make_async_copy(buf.at[pl.ds(0, n - 1)], buf.at[pl.ds(0, n - 1)], ar_send.at[which]).wait()

    all_to_one(packed, ar1, mx, line, 0)

    loads[5].wait()
    route()
    pl.semaphore_wait(ready, len(line))
    exchange(tx, rx)
    loads[6].wait()
    pack_halo(prev, sy_i, sz_i, iy, 0)
    prev_halo = send_halo(1, prev, *inner, 0)
    all_to_one(all_arrived(ar1, 0), ar2, my * ngz + mz, layer, 1)
    loads[7].wait()
    loads[8].wait()
    inv[...] = 1.0 / (6.0 + idiag[...])
    v = prev[...]
    p1[...] = source[...] + near_sum(v, iy)
    for c in prev_halo:
        c.wait_recv()
    p1[...] += far_sum(v.shape, hx_i[0], hy_i[0], hz_i[0], at_ends)

    mu_rows = all_arrived(ar2, 1)
    mu = [(mu_rows[k : k + 1], mu_rows[4 + k : 5 + k]) for k in range(4)]
    a0 = mu[0][0] / mu[1][0]
    rr1 = dd_add(mu[0], dd_times(dd_add(dd_times(mu[2], a0), (-2.0 * mu[1][0], -2.0 * mu[1][1])), a0))
    rr1 = rr1[0] + rr1[1]
    beta = rr1 / mu[0][0]
    g = 1.0 + beta
    curve = dd_times(dd_add(dd_times(mu[1], g), dd_times(mu[2], -2.0 * a0)), g)
    curve = dd_add(curve, dd_times(dd_times(mu[3], a0), a0))
    a1 = rr1 / (curve[0] + curve[1])
    c0, c1 = (a0 + a1 * g)[:, :1], (-a0 * a1)[:, :1]
    a0, a1, beta = a0[:, :1], a1[:, :1], beta[:, :1]

    scatter(c0, c1)
    added = acc[pl.ds(0, ni)] + acc[pl.ds(ni, ni)]
    p1[...] = (p1[...] + added) * inv[...]
    pack_halo(p1, sy_i, sz_i, iy, 1)
    last = send_halo(3, p1, *inner, 1)
    r, q = right[...], q0[...]
    r1 = r - a0 * q
    x_out[...] = a0 * r + a1 * (r1 + beta * r)
    res_out[...] = r1 - a1 * ((q - a0 * q1[...]) + beta * q)
    stores = [
        pltpu.make_async_copy(x_out, x_hbm, store_sem.at[0]),
        pltpu.make_async_copy(res_out, res_hbm, store_sem.at[1]),
    ]
    for c in stores:
        c.start()
    near = source[...] + added + near_sum(p1[...], iy)
    for c in last:
        c.wait_recv()
    p_out[...] = (near + far_sum(near.shape, hx_i[1], hy_i[1], hz_i[1], at_ends)) * inv[...]
    c = pltpu.make_async_copy(p_out, p_hbm, store_sem.at[2])
    c.start()
    stores.append(c)
    for c in first + prev_halo + second + last:
        c.wait_send()
    exchange_sent(tx)
    all_sent(ar1, 0)
    all_sent(ar2, 1)
    for c in stores:
        c.wait()


def hand_out(x, res, p, x_hbm, res_hbm, p_hbm, x_v, res_v, p_v, sem):
    held = ((p, p_v, p_hbm), (x, x_v, x_hbm), (res, res_v, res_hbm))
    into = [pltpu.make_async_copy(a, b, sem.at[0, i]) for i, (a, b, _) in enumerate(held)]
    out = [pltpu.make_async_copy(b, c, sem.at[1, i]) for i, (_, b, c) in enumerate(held)]
    for c in into:
        c.start()
    for c, d in zip(into, out):
        c.wait()
        d.start()
    for d in out:
        d.wait()


def solution(mesh):
    ngx, ngy, ngz = (mesh.shape[a] for a in ("gx", "gy", "gz"))
    groups = ngx * ngy

    def per_device(right, odiag, nodes, weights, dest, cell, prev, source, idiag):
        cx, cy, nz = right.shape
        ix, iy, nzi = source.shape
        points = nodes.shape[0]
        cap = 2 * points // groups
        no, ni = cx * cy, ix * iy
        v = pltpu.VMEM
        dma = pltpu.SemaphoreType.DMA
        scratch = [
            v((no, nz), F32), v((no, nz), F32), v((1, points), I32), v((8, points), F32), v((1, points), I32),
            v((1, points), I32), v((ni, nzi), F32), v((ni, nzi), F32), v((ni, nzi), F32), dma((9,)),
            v((no, nz), F32), v((no, nz), F32), v((ni, nzi), F32), v((no, nz), F32), v((no, nz), F32), v((ni, nzi), F32), dma((3,)),
            v((2, 2, cy, nz), F32), v((2, 2, cx, nz), F32), v((2, 2, 8, LANE), F32), v((2, 2, cx, nz), F32), v((2, 2, 8, LANE), F32),
            v((2, 2, iy, nzi), F32), v((2, 2, ix, nzi), F32), v((2, 2, 8, LANE), F32), v((2, 2, ix, nzi), F32), v((2, 2, 8, LANE), F32),
            dma((4, 6)), dma((4, 6)),
            v((ngx, 8, LANE), F32), v((ngy * ngz, 8, LANE), F32), dma((2,)), dma((2,)),
            v((groups, 1, 3 * cap), F32), v((groups, 1, 3 * cap), F32), dma(()), dma((4,)), pltpu.SemaphoreType.REGULAR,
            v((1, points), F32), v((groups, BLK), F32), v((4 * no, nz), BF16), v((1, points), F32), v((1, points), F32),
            v((6 * groups, cap), F32), v((2 * ni, nzi), F32), v((ni, nzi), F32),
        ]
        x, res, p = pl.pallas_call(
            functools.partial(kernel, (ngx, ngy, ngz, cy, iy)),
            out_shape=(
                jax.ShapeDtypeStruct((no, nz), F32),
                jax.ShapeDtypeStruct((no, nz), F32),
                jax.ShapeDtypeStruct((ni, nzi), F32),
            ),
            in_specs=[pl.BlockSpec(memory_space=pl.ANY)] * 9,
            out_specs=[pl.BlockSpec(memory_space=pl.ANY)] * 3,
            scratch_shapes=scratch,
            compiler_params=pltpu.CompilerParams(
                collective_id=0, has_side_effects=True, vmem_limit_bytes=56 * 2**20
            ),
        )(
            right.reshape(no, nz), odiag.reshape(no, nz), nodes.reshape(1, points), weights,
            dest.reshape(1, points), cell.reshape(1, points), prev.reshape(ni, nzi),
            source.reshape(ni, nzi), idiag.reshape(ni, nzi),
        )
        x, res, p = pl.pallas_call(
            hand_out,
            out_shape=tuple(jax.ShapeDtypeStruct(a.shape, F32) for a in (x, res, p)),
            in_specs=[pl.BlockSpec(memory_space=pl.ANY)] * 3,
            out_specs=[pl.BlockSpec(memory_space=pl.ANY)] * 3,
            scratch_shapes=[v((no, nz), F32), v((no, nz), F32), v((ni, nzi), F32), dma((2, 3))],
            compiler_params=pltpu.CompilerParams(vmem_limit_bytes=60 * 2**20),
        )(x, res, p)
        return x.reshape(cx, cy, nz), res.reshape(cx, cy, nz), p.reshape(ix, iy, nzi)

    block = P("gx", "gy", "gz")
    every = ("gx", "gy", "gz")
    return jax.shard_map(
        per_device,
        mesh=mesh,
        in_specs=(block, block, P(every), P(None, every), P(every, None), P(every), block, block, block),
        out_specs=(block, block, block),
        check_vma=False,
    )
```

```python
import functools

import jax
import jax.numpy as jnp
from jax import lax
from jax.experimental import pallas as pl
from jax.experimental.pallas import tpu as pltpu
from jax.sharding import PartitionSpec as P

MESH = pl.DeviceIdType.MESH
F32 = jnp.float32
BF16 = jnp.bfloat16
I32 = jnp.int32
LANE = 128
BLK = 256


def iota(shape, dim):
    return lax.broadcasted_iota(I32, shape, dim)


def halves(x):
    hi = x.astype(BF16).astype(F32)
    return hi, x - hi


def nt(a, b):
    return lax.dot_general(a, b, (((1,), (1,)), ((), ())), preferred_element_type=F32)


def nn(a, b):
    return lax.dot_general(a, b, (((1,), (0,)), ((), ())), preferred_element_type=F32)


def two_sum(a, b):
    s = a + b
    t = s - a
    return s, (a - (s - t)) + (b - t)


def two_prod(a, b):
    p = a * b
    ca, cb = 4097.0 * a, 4097.0 * b
    ah, bh = ca - (ca - a), cb - (cb - b)
    al, bl = a - ah, b - bh
    return p, ((ah * bh - p) + ah * bl + al * bh) + al * bl


def dd_times(x, f):
    p, e = two_prod(x[0], f)
    return two_sum(p, e + x[1] * f)


def dd_add(x, y):
    s, e = two_sum(x[0], y[0])
    return two_sum(s, e + (x[1] + y[1]))


def column(v, at):
    groups = v.shape[0] // 8
    tile = at // LANE * LANE
    lanes = v[:, tile : tile + LANE].reshape(groups, 8, LANE)
    spread = jnp.broadcast_to(lanes[:, :, at - tile : at - tile + 1], (groups, 8, LANE))
    keep = iota((groups, 8, LANE), 2) == iota((groups, 8, LANE), 0)
    return jnp.sum(jnp.where(keep, spread, 0.0), axis=0)


def uncolumn(c, rows):
    groups = rows // 8
    keep = iota((groups, 8, LANE), 2) == iota((groups, 8, LANE), 0)
    picked = jnp.where(keep, jnp.broadcast_to(c[None], (groups, 8, LANE)), 0.0)
    return jnp.sum(picked, axis=2, keepdims=True).reshape(rows, 1)


def near_sum(v, ny):
    rows, nz = v.shape
    zero = jnp.zeros((ny, nz), F32)
    total = jnp.concatenate([zero, v[: rows - ny]], axis=0) + jnp.concatenate([v[ny:], zero], axis=0)
    in_plane = iota((rows, nz), 0) % ny
    lane = iota((rows, nz), 1)
    total = total + jnp.where(in_plane == 0, 0.0, pltpu.roll(v, 1, 0))
    total = total + jnp.where(in_plane == ny - 1, 0.0, pltpu.roll(v, rows - 1, 0))
    total = total + jnp.where(lane == 0, 0.0, pltpu.roll(v, 1, 1))
    return total + jnp.where(lane == nz - 1, 0.0, pltpu.roll(v, nz - 1, 1))


def far_sum(shape, halo_x, halo_y, halo_z, at_ends):
    rows, nz = shape
    ny = halo_x.shape[1]
    planes = rows // ny
    first_x, last_x, first_y, last_y, first_z, last_z = at_ends
    low = jnp.where(first_x, 0.0, halo_x[0])
    high = jnp.where(last_x, 0.0, halo_x[1])
    total = jnp.concatenate([low, jnp.zeros((rows - 2 * ny, nz), F32), high], axis=0)
    in_plane = iota((rows, nz), 0) % ny
    lane = iota((rows, nz), 1)

    def rows_of(h):
        return jnp.broadcast_to(h[:, None, :], (planes, ny, nz)).reshape(rows, nz)

    total = total + jnp.where(in_plane == 0, rows_of(jnp.where(first_y, 0.0, halo_y[0])), 0.0)
    total = total + jnp.where(in_plane == ny - 1, rows_of(jnp.where(last_y, 0.0, halo_y[1])), 0.0)
    total = total + jnp.where(lane == 0, uncolumn(jnp.where(first_z, 0.0, halo_z[0]), rows), 0.0)
    return total + jnp.where(lane == nz - 1, uncolumn(jnp.where(last_z, 0.0, halo_z[1]), rows), 0.0)


def field_of(x):
    nr, nz = x.shape
    ahead = pltpu.roll(x, nz - 1, 1)
    ahead = jnp.where(iota((nr, nz), 1) == nz - 1, pltpu.roll(ahead, nr - 1, 0), ahead)
    hi, lo = halves(jnp.concatenate([x, ahead], axis=0))
    return jnp.concatenate([hi, lo], axis=0).astype(BF16)


def hot_bf16(ids, wanted, value):
    return jnp.where(ids == wanted.astype(BF16), jnp.broadcast_to(value.astype(BF16), ids.shape), jnp.zeros(ids.shape, BF16))


def interpolate(field, n, w, cy, nz):
    nr = field.shape[0] // 4
    planes, parts, blk = nr // cy, cy // 8, n.shape[1]
    row = n // nz
    a0 = jnp.broadcast_to(row // cy, (8, blk))
    b0 = jnp.broadcast_to(row % cy, (8, blk))
    column_hot = hot_bf16(iota((nz, blk), 0).astype(BF16), n % nz, jnp.ones((1, blk), F32))
    got = nn(field, column_hot)
    got = got[: 2 * nr] + got[2 * nr :]
    here = [a0 == a for a in range(planes - 1)]

    def pick(dc, part, ahead):
        def at(a):
            s = dc * nr + min(a + ahead, planes - 1) * cy + part * 8
            return got[s : s + 8]

        v = at(planes - 2)
        for a in range(planes - 3, -1, -1):
            v = jnp.where(here[a], at(a), v)
        return v

    sub = iota((8, blk), 0)
    total = jnp.zeros((8, blk), F32)
    for dc in range(2):
        picked = [[pick(dc, part, ahead) for part in range(parts)] for ahead in range(2)] + [[pick(dc, 0, 2)]]
        for da in range(2):
            wa, wb = w(da * 4 + dc), w(da * 4 + 2 + dc)
            for part in range(parts):
                wt = jnp.where(b0 == sub + 8 * part, wa, jnp.where(b0 + 1 == sub + 8 * part, wb, 0.0))
                total = total + wt * picked[da][part]
            total = total + jnp.where(b0 + 1 == sub + cy, wb, 0.0) * picked[da + 1][0]
    return jnp.sum(total, axis=0, keepdims=True)


def kernel(
    sizes,
    right_hbm, odiag_hbm, nodes_hbm, weights_hbm, dest_hbm, cell_hbm, prev_hbm, source_hbm, idiag_hbm,
    x_out, res_out, p_out,
    right, odiag, nodes, weights, dest, cell, prev, source, idiag, load_sem,
    q0, q1, p1,
    hx_o, hy_o, hz_o, sy_o, sz_o, hx_i, hy_i, hz_i, sy_i, sz_i, halo_send, halo_recv,
    ar1, ar2, ar_send, ar_recv,
    tx, rx, a2a_send, a2a_recv, ready,
    rank, carry, field, handed_r, handed_q, routed, acc, inv,
):
    ngx, ngy, ngz, cy, iy = sizes
    mx, my, mz = lax.axis_index("gx"), lax.axis_index("gy"), lax.axis_index("gz")
    groups = ngx * ngy
    me = mx * ngy + my
    points = nodes.shape[1]
    blocks = points // BLK
    cap = tx.shape[2] // 3
    at_ends = (mx == 0, mx == ngx - 1, my == 0, my == ngy - 1, mz == 0, mz == ngz - 1)

    barrier = pltpu.get_barrier_semaphore()

    def peer(k):
        t = lax.rem(me + k, groups)
        return t, (t // ngy, lax.rem(t, ngy), mz)

    loads = []
    for i, (a, b) in enumerate(
        ((right_hbm, right), (dest_hbm, dest), (nodes_hbm, nodes), (weights_hbm, weights), (odiag_hbm, odiag),
         (cell_hbm, cell), (prev_hbm, prev), (source_hbm, source), (idiag_hbm, idiag))
    ):
        c = pltpu.make_async_copy(a, b, load_sem.at[i])
        c.start()
        loads.append(c)
    side = [(a, b) for a in range(ngy) for b in range(ngz) if (a, b) != (0, 0)]
    side.sort(key=lambda t: -(min(t[0], ngy - t[0]) + min(t[1], ngz - t[1])))
    along = sorted(range(1, ngx), key=lambda k: -min(k, ngx - k))

    def beside(a, b):
        return (mx, lax.rem(my + a, ngy), lax.rem(mz + b, ngz))

    line = [(lax.rem(mx + k, ngx), my, mz) for k in along]
    layer = [beside(a, b) for a, b in side]
    for to in line + layer:
        pl.semaphore_signal(barrier, inc=1, device_id=to, device_id_type=MESH)

    up = ((lax.rem(mx + 1, ngx), my, mz), (mx, lax.rem(my + 1, ngy), mz), (mx, my, lax.rem(mz + 1, ngz)))
    down = (
        (lax.rem(mx + ngx - 1, ngx), my, mz),
        (mx, lax.rem(my + ngy - 1, ngy), mz),
        (mx, my, lax.rem(mz + ngz - 1, ngz)),
    )

    def pack_halo(src, sy, sz, ny, slot):
        rows, nz = src.shape
        v = src[...]
        solid = v.reshape(rows // ny, ny, nz)
        sy[slot, 0] = solid[:, ny - 1, :]
        sy[slot, 1] = solid[:, 0, :]
        sz[slot, 0] = column(v, nz - 1)
        sz[slot, 1] = column(v, 0)

    def send_halo(which, src, hx, hy, hz, sy, sz, slot):
        rows = src.shape[0]
        ny = hx.shape[2]
        copies = []

        def send(j, a, b, to):
            c = pltpu.make_async_remote_copy(
                a, b, halo_send.at[which, j], halo_recv.at[which, j], device_id=to, device_id_type=MESH
            )
            c.start()
            copies.append(c)

        send(0, src.at[pl.ds(rows - ny, ny)], hx.at[slot, 0], up[0])
        send(1, src.at[pl.ds(0, ny)], hx.at[slot, 1], down[0])
        send(2, sy.at[slot, 0], hy.at[slot, 0], up[1])
        send(3, sy.at[slot, 1], hy.at[slot, 1], down[1])
        send(4, sz.at[slot, 0], hz.at[slot, 0], up[2])
        send(5, sz.at[slot, 1], hz.at[slot, 1], down[2])
        return copies

    outer = (hx_o, hy_o, hz_o, sy_o, sz_o)
    inner = (hx_i, hy_i, hz_i, sy_i, sz_i)
    nz = right.shape[1]

    def rank_points():
        low = iota((BLK, BLK), 0) < iota((BLK, BLK), 1)
        tri = jnp.concatenate([jnp.where(low, 1.0, 0.0), jnp.ones((BLK, BLK), F32)], axis=1).astype(BF16)
        carry[...] = jnp.zeros_like(carry)
        step = next(s for s in (16, 4, 1) if blocks % s == 0)
        ids = iota((groups, BLK), 0)
        one = jnp.ones((1, BLK), F32)

        def rank_step(j, _):
            seen = carry[...]
            for b in range(step):
                at = pl.ds(pl.multiple_of((j * step + b) * BLK, BLK), BLK)
                name = dest[:, at]
                part = nn(hot_bf16(ids.astype(BF16), name, one), tri)
                rank[:, at] = jnp.sum(jnp.where(ids == name, part[:, :BLK] + seen, 0.0), axis=0, keepdims=True)
                seen = seen + part[:, BLK:]
            carry[...] = seen
            return 0

        lax.fori_loop(0, blocks // step, rank_step, 0)

    many = next(s for s in (16, 4, 1) if blocks % s == 0)

    def interpolate_all(handed, first, end):
        def go(j, _):
            for b in range(many):
                at = pl.ds(pl.multiple_of((j * many + b) * BLK, BLK), BLK)
                handed[:, at] = interpolate(field[...], nodes[:, at], lambda k: weights[k : k + 1, at], cy, nz)
            return 0

        lax.fori_loop(first, end, go, 0)

    def route():
        ids = iota((groups, BLK), 0).astype(BF16)
        slots = iota((cap, BLK), 0).astype(BF16)
        one = jnp.ones((1, BLK), F32)
        routed[...] = jnp.zeros_like(routed)

        def go(j, _):
            part = jnp.zeros(routed.shape, F32)
            for b in range(many):
                at = pl.ds(pl.multiple_of((j * many + b) * BLK, BLK), BLK)
                c = cell[:, at]
                values = (*halves(handed_r[:, at]), *halves(handed_q[:, at]), (c // 256).astype(F32), (c % 256).astype(F32))
                left = jnp.concatenate([hot_bf16(ids, dest[:, at], v) for v in values], axis=0)
                part = part + nt(left, hot_bf16(slots, rank[:, at], one))
            routed[...] += part
            return 0

        lax.fori_loop(0, blocks // many, go, 0)
        rows = [routed[pl.ds(i * groups, groups)] for i in range(6)]
        tx[...] = jnp.concatenate([rows[0] + rows[1], rows[2] + rows[3], rows[4] * 256.0 + rows[5]], axis=1).reshape(
            groups, 1, 3 * cap
        )

    middle = groups // 2
    batch = next(s for s in (16, 8, 4, 2, 1) if groups % s == 0)

    def offset(i):
        half = (i + 1) // 2
        return middle + jnp.where(lax.rem(i, 2) == 1, half, -half)

    def exchange(src, dst):
        def go(i, _):
            t, to = peer(offset(i))
            pltpu.make_async_remote_copy(
                src.at[t], dst.at[me], a2a_send, a2a_recv.at[i // batch], device_id=to, device_id_type=MESH
            ).start()
            return 0

        lax.fori_loop(0, groups - 1, go, 0)
        pltpu.make_async_copy(src.at[me], dst.at[me], a2a_recv.at[groups // batch - 1]).start()

    def exchanged(dst, j):
        pltpu.make_async_copy(dst.at[pl.ds(0, batch)], dst.at[pl.ds(0, batch)], a2a_recv.at[j]).wait()

    def exchange_sent(src):
        all_but_one = pl.ds(0, groups - 1)
        pltpu.make_async_copy(src.at[all_but_one], src.at[all_but_one], a2a_send).wait()

    ni, nzi = source.shape

    def scatter(c0, c1):
        rows_id = iota((ni, cap), 0).astype(BF16)
        cols_id = iota((nzi, cap), 0).astype(BF16)
        one = jnp.ones((1, cap), F32)
        acc[...] = jnp.zeros_like(acc)

        def go(j, _):
            exchanged(rx, j)
            part = jnp.zeros(acc.shape, F32)
            for b in range(batch):
                got = rx[lax.rem(me + 2 * groups - offset(j * batch + b), groups)]
                c = got[:, 2 * cap :].astype(I32)
                hi, lo = halves(c0 * got[:, :cap] + c1 * got[:, cap : 2 * cap])
                left = jnp.concatenate([hot_bf16(rows_id, c // nzi, hi), hot_bf16(rows_id, c // nzi, lo)], axis=0)
                part = part + nt(left, hot_bf16(cols_id, c % nzi, one))
            acc[...] += part
            return 0

        lax.fori_loop(0, groups // batch, go, 0)

    loads[0].wait()
    pack_halo(right, sy_o, sz_o, cy, 0)
    field[...] = field_of(right[...])
    loads[1].wait()
    rank_points()
    pl.semaphore_wait(barrier, len(line) + len(layer))
    first = send_halo(0, right, *outer, 0)
    for to in line:
        pl.semaphore_signal(ready, inc=1, device_id=to, device_id_type=MESH)
    loads[2].wait()
    loads[3].wait()
    interpolate_all(handed_r, 0, blocks // many)

    loads[4].wait()
    r = right[...]
    near = (6.0 + odiag[...]) * r - near_sum(r, cy)
    for c in first:
        c.wait_recv()
    q0[...] = near - far_sum(r.shape, hx_o[0], hy_o[0], hz_o[0], at_ends)
    pack_halo(q0, sy_o, sz_o, cy, 1)
    second = send_halo(2, q0, *outer, 1)
    field[...] = field_of(q0[...])
    interpolate_all(handed_q, 0, blocks // many)

    q = q0[...]
    near = (6.0 + odiag[...]) * q - near_sum(q, cy)
    for c in second:
        c.wait_recv()
    q1[...] = near - far_sum(q.shape, hx_o[1], hy_o[1], hz_o[1], at_ends)
    row8 = iota((8, LANE), 0)
    packed = jnp.zeros((8, LANE), F32)
    r, qq = right[...], q1[...]
    for k, (a, b) in enumerate(((r, r), (r, q), (q, q), (q, qq))):
        s = jnp.sum((a * b).reshape(-1, 8, nz), axis=0)
        t = s[:, :LANE]
        for m in range(LANE, nz, LANE):
            t = t + s[:, m : m + LANE]
        packed = jnp.where(row8 == k, jnp.sum(t, axis=0, keepdims=True), packed)
    packed = jnp.broadcast_to(jnp.sum(packed, axis=1, keepdims=True), (8, LANE))

    def all_to_one(value, buf, mine, partners, which):
        buf[pl.ds(mine, 1)] = value[None]
        for to in partners:
            pltpu.make_async_remote_copy(
                buf.at[mine], buf.at[mine], ar_send.at[which], ar_recv.at[which], device_id=to, device_id_type=MESH
            ).start()

    def all_arrived(buf, which):
        n = buf.shape[0]
        pltpu.make_async_copy(buf.at[pl.ds(0, n - 1)], buf.at[pl.ds(0, n - 1)], ar_recv.at[which]).wait()
        s, e = buf[0], jnp.zeros((8, LANE), F32)
        for i in range(1, n):
            s, d = two_sum(s, buf[i])
            e = e + d
        return s + jnp.where(row8 >= 4, pltpu.roll(e, 4, 0), 0.0)

    def all_sent(buf, which):
        n = buf.shape[0]
        pltpu.make_async_copy(buf.at[pl.ds(0, n - 1)], buf.at[pl.ds(0, n - 1)], ar_send.at[which]).wait()

    all_to_one(packed, ar1, mx, line, 0)

    loads[5].wait()
    route()
    pl.semaphore_wait(ready, len(line))
    exchange(tx, rx)
    loads[6].wait()
    pack_halo(prev, sy_i, sz_i, iy, 0)
    prev_halo = send_halo(1, prev, *inner, 0)
    all_to_one(all_arrived(ar1, 0), ar2, my * ngz + mz, layer, 1)
    loads[7].wait()
    loads[8].wait()
    inv[...] = 1.0 / (6.0 + idiag[...])
    v = prev[...]
    p1[...] = source[...] + near_sum(v, iy)
    for c in prev_halo:
        c.wait_recv()
    p1[...] += far_sum(v.shape, hx_i[0], hy_i[0], hz_i[0], at_ends)

    mu_rows = all_arrived(ar2, 1)
    mu = [(mu_rows[k : k + 1], mu_rows[4 + k : 5 + k]) for k in range(4)]
    a0 = mu[0][0] / mu[1][0]
    rr1 = dd_add(mu[0], dd_times(dd_add(dd_times(mu[2], a0), (-2.0 * mu[1][0], -2.0 * mu[1][1])), a0))
    rr1 = rr1[0] + rr1[1]
    beta = rr1 / mu[0][0]
    g = 1.0 + beta
    curve = dd_times(dd_add(dd_times(mu[1], g), dd_times(mu[2], -2.0 * a0)), g)
    curve = dd_add(curve, dd_times(dd_times(mu[3], a0), a0))
    a1 = rr1 / (curve[0] + curve[1])
    c0, c1 = (a0 + a1 * g)[:, :1], (-a0 * a1)[:, :1]
    a0, a1, beta = a0[:, :1], a1[:, :1], beta[:, :1]

    scatter(c0, c1)
    added = acc[pl.ds(0, ni)] + acc[pl.ds(ni, ni)]
    p1[...] = (p1[...] + added) * inv[...]
    pack_halo(p1, sy_i, sz_i, iy, 1)
    last = send_halo(3, p1, *inner, 1)
    r, q = right[...], q0[...]
    r1 = r - a0 * q
    x_out[...] = a0 * r + a1 * (r1 + beta * r)
    res_out[...] = r1 - a1 * ((q - a0 * q1[...]) + beta * q)
    near = source[...] + added + near_sum(p1[...], iy)
    for c in last:
        c.wait_recv()
    p_out[...] = (near + far_sum(near.shape, hx_i[1], hy_i[1], hz_i[1], at_ends)) * inv[...]
    for c in first + prev_halo + second + last:
        c.wait_send()
    exchange_sent(tx)
    all_sent(ar1, 0)
    all_sent(ar2, 1)


def hand_out(x, res, p, x_hbm, res_hbm, p_hbm, sem):
    pairs = ((p, p_hbm), (x, x_hbm), (res, res_hbm))
    copies = [pltpu.make_async_copy(a, b, sem.at[i]) for i, (a, b) in enumerate(pairs)]
    for c in copies:
        c.start()
    for c in copies:
        c.wait()


def solution(mesh):
    ngx, ngy, ngz = (mesh.shape[a] for a in ("gx", "gy", "gz"))
    groups = ngx * ngy

    def per_device(right, odiag, nodes, weights, dest, cell, prev, source, idiag):
        cx, cy, nz = right.shape
        ix, iy, nzi = source.shape
        points = nodes.shape[0]
        cap = 2 * points // groups
        no, ni = cx * cy, ix * iy
        v = pltpu.VMEM
        dma = pltpu.SemaphoreType.DMA
        scratch = [
            v((no, nz), F32), v((no, nz), F32), v((1, points), I32), v((8, points), F32), v((1, points), I32),
            v((1, points), I32), v((ni, nzi), F32), v((ni, nzi), F32), v((ni, nzi), F32), dma((9,)),
            v((no, nz), F32), v((no, nz), F32), v((ni, nzi), F32),
            v((2, 2, cy, nz), F32), v((2, 2, cx, nz), F32), v((2, 2, 8, LANE), F32), v((2, 2, cx, nz), F32), v((2, 2, 8, LANE), F32),
            v((2, 2, iy, nzi), F32), v((2, 2, ix, nzi), F32), v((2, 2, 8, LANE), F32), v((2, 2, ix, nzi), F32), v((2, 2, 8, LANE), F32),
            dma((4, 6)), dma((4, 6)),
            v((ngx, 8, LANE), F32), v((ngy * ngz, 8, LANE), F32), dma((2,)), dma((2,)),
            v((groups, 1, 3 * cap), F32), v((groups, 1, 3 * cap), F32), dma(()), dma((4,)), pltpu.SemaphoreType.REGULAR,
            v((1, points), F32), v((groups, BLK), F32), v((4 * no, nz), BF16), v((1, points), F32), v((1, points), F32),
            v((6 * groups, cap), F32), v((2 * ni, nzi), F32), v((ni, nzi), F32),
        ]
        x, res, p = pl.pallas_call(
            functools.partial(kernel, (ngx, ngy, ngz, cy, iy)),
            out_shape=(v((no, nz), F32), v((no, nz), F32), v((ni, nzi), F32)),
            in_specs=[pl.BlockSpec(memory_space=pl.ANY)] * 9,
            out_specs=[pl.BlockSpec(memory_space=pltpu.VMEM)] * 3,
            scratch_shapes=scratch,
            compiler_params=pltpu.CompilerParams(
                collective_id=0, has_side_effects=True, vmem_limit_bytes=56 * 2**20
            ),
        )(
            right.reshape(no, nz), odiag.reshape(no, nz), nodes.reshape(1, points), weights,
            dest.reshape(1, points), cell.reshape(1, points), prev.reshape(ni, nzi),
            source.reshape(ni, nzi), idiag.reshape(ni, nzi),
        )
        x, res, p = pl.pallas_call(
            hand_out,
            out_shape=tuple(jax.ShapeDtypeStruct(a.shape, F32) for a in (x, res, p)),
            in_specs=[pl.BlockSpec(memory_space=pltpu.VMEM)] * 3,
            out_specs=[pl.BlockSpec(memory_space=pl.ANY)] * 3,
            scratch_shapes=[dma((3,))],
            compiler_params=pltpu.CompilerParams(vmem_limit_bytes=32 * 2**20),
        )(x, res, p)
        return x.reshape(cx, cy, nz), res.reshape(cx, cy, nz), p.reshape(ix, iy, nzi)

    block = P("gx", "gy", "gz")
    every = ("gx", "gy", "gz")
    return jax.shard_map(
        per_device,
        mesh=mesh,
        in_specs=(block, block, P(every), P(None, every), P(every, None), P(every), block, block, block),
        out_specs=(block, block, block),
        check_vma=False,
    )
```

```python
import functools

import jax
import jax.numpy as jnp
from jax import lax
from jax.experimental import pallas as pl
from jax.experimental.pallas import tpu as pltpu
from jax.sharding import PartitionSpec as P

MESH = pl.DeviceIdType.MESH
F32 = jnp.float32
BF16 = jnp.bfloat16
I32 = jnp.int32
LANE = 128
BLK = 256


def iota(shape, dim):
    return lax.broadcasted_iota(I32, shape, dim)


def halves(x):
    hi = x.astype(BF16).astype(F32)
    return hi, x - hi


def nt(a, b):
    return lax.dot_general(a, b, (((1,), (1,)), ((), ())), preferred_element_type=F32)


def nn(a, b):
    return lax.dot_general(a, b, (((1,), (0,)), ((), ())), preferred_element_type=F32)


def two_sum(a, b):
    s = a + b
    t = s - a
    return s, (a - (s - t)) + (b - t)


def two_prod(a, b):
    p = a * b
    ca, cb = 4097.0 * a, 4097.0 * b
    ah, bh = ca - (ca - a), cb - (cb - b)
    al, bl = a - ah, b - bh
    return p, ((ah * bh - p) + ah * bl + al * bh) + al * bl


def dd_times(x, f):
    p, e = two_prod(x[0], f)
    return two_sum(p, e + x[1] * f)


def dd_add(x, y):
    s, e = two_sum(x[0], y[0])
    return two_sum(s, e + (x[1] + y[1]))


def column(v, at):
    groups = v.shape[0] // 8
    tile = at // LANE * LANE
    lanes = v[:, tile : tile + LANE].reshape(groups, 8, LANE)
    spread = jnp.broadcast_to(lanes[:, :, at - tile : at - tile + 1], (groups, 8, LANE))
    keep = iota((groups, 8, LANE), 2) == iota((groups, 8, LANE), 0)
    return jnp.sum(jnp.where(keep, spread, 0.0), axis=0)


def uncolumn(c, rows):
    groups = rows // 8
    keep = iota((groups, 8, LANE), 2) == iota((groups, 8, LANE), 0)
    picked = jnp.where(keep, jnp.broadcast_to(c[None], (groups, 8, LANE)), 0.0)
    return jnp.sum(picked, axis=2, keepdims=True).reshape(rows, 1)


def near_sum(v, ny):
    rows, nz = v.shape
    zero = jnp.zeros((ny, nz), F32)
    total = jnp.concatenate([zero, v[: rows - ny]], axis=0) + jnp.concatenate([v[ny:], zero], axis=0)
    in_plane = iota((rows, nz), 0) % ny
    lane = iota((rows, nz), 1)
    total = total + jnp.where(in_plane == 0, 0.0, pltpu.roll(v, 1, 0))
    total = total + jnp.where(in_plane == ny - 1, 0.0, pltpu.roll(v, rows - 1, 0))
    total = total + jnp.where(lane == 0, 0.0, pltpu.roll(v, 1, 1))
    return total + jnp.where(lane == nz - 1, 0.0, pltpu.roll(v, nz - 1, 1))


def far_sum(shape, halo_x, halo_y, halo_z, at_ends):
    rows, nz = shape
    ny = halo_x.shape[1]
    planes = rows // ny
    first_x, last_x, first_y, last_y, first_z, last_z = at_ends
    low = jnp.where(first_x, 0.0, halo_x[0])
    high = jnp.where(last_x, 0.0, halo_x[1])
    total = jnp.concatenate([low, jnp.zeros((rows - 2 * ny, nz), F32), high], axis=0)
    in_plane = iota((rows, nz), 0) % ny
    lane = iota((rows, nz), 1)

    def rows_of(h):
        return jnp.broadcast_to(h[:, None, :], (planes, ny, nz)).reshape(rows, nz)

    total = total + jnp.where(in_plane == 0, rows_of(jnp.where(first_y, 0.0, halo_y[0])), 0.0)
    total = total + jnp.where(in_plane == ny - 1, rows_of(jnp.where(last_y, 0.0, halo_y[1])), 0.0)
    total = total + jnp.where(lane == 0, uncolumn(jnp.where(first_z, 0.0, halo_z[0]), rows), 0.0)
    return total + jnp.where(lane == nz - 1, uncolumn(jnp.where(last_z, 0.0, halo_z[1]), rows), 0.0)


def field_of(x):
    nr, nz = x.shape
    ahead = pltpu.roll(x, nz - 1, 1)
    ahead = jnp.where(iota((nr, nz), 1) == nz - 1, pltpu.roll(ahead, nr - 1, 0), ahead)
    hi, lo = halves(jnp.concatenate([x, ahead], axis=0))
    return jnp.concatenate([hi, lo], axis=0).astype(BF16)


def hot_bf16(ids, wanted, value):
    return jnp.where(ids == wanted.astype(BF16), jnp.broadcast_to(value.astype(BF16), ids.shape), jnp.zeros(ids.shape, BF16))


def interpolate(field, n, w, cy, nz):
    nr = field.shape[0] // 4
    planes, parts, blk = nr // cy, cy // 8, n.shape[1]
    row = n // nz
    a0 = jnp.broadcast_to(row // cy, (8, blk))
    b0 = jnp.broadcast_to(row % cy, (8, blk))
    column_hot = hot_bf16(iota((nz, blk), 0).astype(BF16), n % nz, jnp.ones((1, blk), F32))
    got = nn(field, column_hot)
    got = got[: 2 * nr] + got[2 * nr :]
    here = [a0 == a for a in range(planes - 1)]

    def pick(dc, part, ahead):
        def at(a):
            s = dc * nr + min(a + ahead, planes - 1) * cy + part * 8
            return got[s : s + 8]

        v = at(planes - 2)
        for a in range(planes - 3, -1, -1):
            v = jnp.where(here[a], at(a), v)
        return v

    sub = iota((8, blk), 0)
    total = jnp.zeros((8, blk), F32)
    for dc in range(2):
        picked = [[pick(dc, part, ahead) for part in range(parts)] for ahead in range(2)] + [[pick(dc, 0, 2)]]
        for da in range(2):
            wa, wb = w(da * 4 + dc), w(da * 4 + 2 + dc)
            for part in range(parts):
                wt = jnp.where(b0 == sub + 8 * part, wa, jnp.where(b0 + 1 == sub + 8 * part, wb, 0.0))
                total = total + wt * picked[da][part]
            total = total + jnp.where(b0 + 1 == sub + cy, wb, 0.0) * picked[da + 1][0]
    return jnp.sum(total, axis=0, keepdims=True)


def kernel(
    sizes,
    right_hbm, odiag_hbm, nodes_hbm, weights_hbm, dest_hbm, cell_hbm, prev_hbm, source_hbm, idiag_hbm,
    x_out, res_out, p_out,
    right, odiag, nodes, weights, dest, cell, prev, source, idiag, load_sem,
    q0, q1, p1,
    hx_o, hy_o, hz_o, sy_o, sz_o, hx_i, hy_i, hz_i, sy_i, sz_i, halo_send, halo_recv,
    ar1, ar2, ar_send, ar_recv,
    tx, rx, a2a_send, a2a_recv, ready,
    rank, carry, field, handed_r, handed_q, routed, acc, inv,
):
    ngx, ngy, ngz, cy, iy = sizes
    mx, my, mz = lax.axis_index("gx"), lax.axis_index("gy"), lax.axis_index("gz")
    groups = ngx * ngy
    me = mx * ngy + my
    points = nodes.shape[1]
    blocks = points // BLK
    cap = tx.shape[2] // 3
    at_ends = (mx == 0, mx == ngx - 1, my == 0, my == ngy - 1, mz == 0, mz == ngz - 1)

    barrier = pltpu.get_barrier_semaphore()

    def peer(k):
        t = lax.rem(me + k, groups)
        return t, (t // ngy, lax.rem(t, ngy), mz)

    loads = []
    for i, (a, b) in enumerate(
        ((right_hbm, right), (dest_hbm, dest), (nodes_hbm, nodes), (weights_hbm, weights), (odiag_hbm, odiag),
         (cell_hbm, cell), (prev_hbm, prev), (source_hbm, source), (idiag_hbm, idiag))
    ):
        c = pltpu.make_async_copy(a, b, load_sem.at[i])
        c.start()
        loads.append(c)
    side = [(a, b) for a in range(ngy) for b in range(ngz) if (a, b) != (0, 0)]
    side.sort(key=lambda t: -(min(t[0], ngy - t[0]) + min(t[1], ngz - t[1])))
    along = sorted(range(1, ngx), key=lambda k: -min(k, ngx - k))

    def beside(a, b):
        return (mx, lax.rem(my + a, ngy), lax.rem(mz + b, ngz))

    line = [(lax.rem(mx + k, ngx), my, mz) for k in along]
    layer = [beside(a, b) for a, b in side]
    for to in line + layer:
        pl.semaphore_signal(barrier, inc=1, device_id=to, device_id_type=MESH)

    up = ((lax.rem(mx + 1, ngx), my, mz), (mx, lax.rem(my + 1, ngy), mz), (mx, my, lax.rem(mz + 1, ngz)))
    down = (
        (lax.rem(mx + ngx - 1, ngx), my, mz),
        (mx, lax.rem(my + ngy - 1, ngy), mz),
        (mx, my, lax.rem(mz + ngz - 1, ngz)),
    )

    def pack_y(src, sy, ny, slot):
        v = src[...]
        solid = v.reshape(v.shape[0] // ny, ny, v.shape[1])
        sy[slot, 0] = solid[:, ny - 1, :]
        sy[slot, 1] = solid[:, 0, :]

    def pack_z(src, sz, slot):
        v = src[...]
        sz[slot, 0] = column(v, v.shape[1] - 1)
        sz[slot, 1] = column(v, 0)

    def send_halo(which, src, hx, hy, hz, sy, sz, slot, packed=False):
        rows = src.shape[0]
        ny = hx.shape[2]
        copies = []

        def send(j, a, b, to):
            c = pltpu.make_async_remote_copy(
                a, b, halo_send.at[which, j], halo_recv.at[which, j], device_id=to, device_id_type=MESH
            )
            c.start()
            copies.append(c)

        send(0, src.at[pl.ds(rows - ny, ny)], hx.at[slot, 0], up[0])
        send(1, src.at[pl.ds(0, ny)], hx.at[slot, 1], down[0])
        if not packed:
            pack_y(src, sy, ny, slot)
        send(2, sy.at[slot, 0], hy.at[slot, 0], up[1])
        send(3, sy.at[slot, 1], hy.at[slot, 1], down[1])
        if not packed:
            pack_z(src, sz, slot)
        send(4, sz.at[slot, 0], hz.at[slot, 0], up[2])
        send(5, sz.at[slot, 1], hz.at[slot, 1], down[2])
        return copies

    outer = (hx_o, hy_o, hz_o, sy_o, sz_o)
    inner = (hx_i, hy_i, hz_i, sy_i, sz_i)
    nz = right.shape[1]

    def rank_points():
        low = iota((BLK, BLK), 0) < iota((BLK, BLK), 1)
        tri = jnp.concatenate([jnp.where(low, 1.0, 0.0), jnp.ones((BLK, BLK), F32)], axis=1).astype(BF16)
        carry[...] = jnp.zeros_like(carry)
        step = next(s for s in (16, 4, 1) if blocks % s == 0)
        ids = iota((groups, BLK), 0)
        one = jnp.ones((1, BLK), F32)

        def rank_step(j, _):
            seen = carry[...]
            for b in range(step):
                at = pl.ds(pl.multiple_of((j * step + b) * BLK, BLK), BLK)
                name = dest[:, at]
                part = nn(hot_bf16(ids.astype(BF16), name, one), tri)
                rank[:, at] = jnp.sum(jnp.where(ids == name, part[:, :BLK] + seen, 0.0), axis=0, keepdims=True)
                seen = seen + part[:, BLK:]
            carry[...] = seen
            return 0

        lax.fori_loop(0, blocks // step, rank_step, 0)

    many = next(s for s in (16, 4, 1) if blocks % s == 0)

    def interpolate_all(handed, first, end):
        def go(j, _):
            for b in range(many):
                at = pl.ds(pl.multiple_of((j * many + b) * BLK, BLK), BLK)
                handed[:, at] = interpolate(field[...], nodes[:, at], lambda k: weights[k : k + 1, at], cy, nz)
            return 0

        lax.fori_loop(first, end, go, 0)

    def route():
        ids = iota((groups, BLK), 0).astype(BF16)
        slots = iota((cap, BLK), 0).astype(BF16)
        one = jnp.ones((1, BLK), F32)
        routed[...] = jnp.zeros_like(routed)

        def go(j, _):
            part = jnp.zeros(routed.shape, F32)
            for b in range(many):
                at = pl.ds(pl.multiple_of((j * many + b) * BLK, BLK), BLK)
                c = cell[:, at]
                values = (*halves(handed_r[:, at]), *halves(handed_q[:, at]), (c // 256).astype(F32), (c % 256).astype(F32))
                left = jnp.concatenate([hot_bf16(ids, dest[:, at], v) for v in values], axis=0)
                part = part + nt(left, hot_bf16(slots, rank[:, at], one))
            routed[...] += part
            return 0

        lax.fori_loop(0, blocks // many, go, 0)
        rows = [routed[pl.ds(i * groups, groups)] for i in range(6)]
        tx[...] = jnp.concatenate([rows[0] + rows[1], rows[2] + rows[3], rows[4] * 256.0 + rows[5]], axis=1).reshape(
            groups, 1, 3 * cap
        )

    middle = groups // 2
    batch = next(s for s in (16, 8, 4, 2, 1) if groups % s == 0)

    def offset(i):
        half = (i + 1) // 2
        return middle + jnp.where(lax.rem(i, 2) == 1, half, -half)

    def exchange(src, dst):
        def go(i, _):
            t, to = peer(offset(i))
            pltpu.make_async_remote_copy(
                src.at[t], dst.at[me], a2a_send, a2a_recv.at[i // batch], device_id=to, device_id_type=MESH
            ).start()
            return 0

        lax.fori_loop(0, groups - 1, go, 0)
        pltpu.make_async_copy(src.at[me], dst.at[me], a2a_recv.at[groups // batch - 1]).start()

    def exchanged(dst, j):
        pltpu.make_async_copy(dst.at[pl.ds(0, batch)], dst.at[pl.ds(0, batch)], a2a_recv.at[j]).wait()

    def exchange_sent(src):
        all_but_one = pl.ds(0, groups - 1)
        pltpu.make_async_copy(src.at[all_but_one], src.at[all_but_one], a2a_send).wait()

    ni, nzi = source.shape

    def scatter(c0, c1):
        rows_id = iota((ni, cap), 0).astype(BF16)
        cols_id = iota((nzi, cap), 0).astype(BF16)
        one = jnp.ones((1, cap), F32)
        acc[...] = jnp.zeros_like(acc)

        def go(j, _):
            exchanged(rx, j)
            part = jnp.zeros(acc.shape, F32)
            for b in range(batch):
                got = rx[lax.rem(me + 2 * groups - offset(j * batch + b), groups)]
                c = got[:, 2 * cap :].astype(I32)
                hi, lo = halves(c0 * got[:, :cap] + c1 * got[:, cap : 2 * cap])
                left = jnp.concatenate([hot_bf16(rows_id, c // nzi, hi), hot_bf16(rows_id, c // nzi, lo)], axis=0)
                part = part + nt(left, hot_bf16(cols_id, c % nzi, one))
            acc[...] += part
            return 0

        lax.fori_loop(0, groups // batch, go, 0)

    loads[0].wait()
    pack_y(right, sy_o, cy, 0)
    pack_z(right, sz_o, 0)
    field[...] = field_of(right[...])
    loads[1].wait()
    rank_points()
    pl.semaphore_wait(barrier, len(line) + len(layer))
    first = send_halo(0, right, *outer, 0, packed=True)
    for to in line:
        pl.semaphore_signal(ready, inc=1, device_id=to, device_id_type=MESH)
    loads[2].wait()
    loads[3].wait()
    interpolate_all(handed_r, 0, blocks // many)

    loads[4].wait()
    r = right[...]
    near = (6.0 + odiag[...]) * r - near_sum(r, cy)
    for c in first:
        c.wait_recv()
    q0[...] = near - far_sum(r.shape, hx_o[0], hy_o[0], hz_o[0], at_ends)
    second = send_halo(2, q0, *outer, 1)
    field[...] = field_of(q0[...])
    interpolate_all(handed_q, 0, blocks // many)

    q = q0[...]
    near = (6.0 + odiag[...]) * q - near_sum(q, cy)
    row8 = iota((8, LANE), 0)

    def folded(a, b):
        t = jnp.sum((a * b).reshape(-1, 8, nz), axis=0)
        t = sum((t[:, m : m + LANE] for m in range(LANE, nz, LANE)), t[:, :LANE])
        return jnp.sum(t, axis=0, keepdims=True)

    r = right[...]
    packed = jnp.zeros((8, LANE), F32)
    for k, (a, b) in enumerate(((r, r), (r, q), (q, q))):
        packed = jnp.where(row8 == k, folded(a, b), packed)
    for c in second:
        c.wait_recv()
    qq = near - far_sum(q.shape, hx_o[1], hy_o[1], hz_o[1], at_ends)
    packed = jnp.where(row8 == 3, folded(q, qq), packed)
    packed = jnp.broadcast_to(jnp.sum(packed, axis=1, keepdims=True), (8, LANE))
    q1[...] = qq

    def all_to_one(value, buf, mine, partners, which):
        buf[pl.ds(mine, 1)] = value[None]
        for to in partners:
            pltpu.make_async_remote_copy(
                buf.at[mine], buf.at[mine], ar_send.at[which], ar_recv.at[which], device_id=to, device_id_type=MESH
            ).start()

    def all_arrived(buf, which):
        n = buf.shape[0]
        pltpu.make_async_copy(buf.at[pl.ds(0, n - 1)], buf.at[pl.ds(0, n - 1)], ar_recv.at[which]).wait()
        terms = [(buf[i], jnp.zeros((8, LANE), F32)) for i in range(n)]
        while len(terms) > 1:
            odd = terms[len(terms) // 2 * 2 :]
            pairs = [(*two_sum(x[0], y[0]), x[1] + y[1]) for x, y in zip(terms[::2], terms[1::2])]
            terms = [(t, d + e) for t, d, e in pairs] + odd
        s, e = terms[0]
        return s + jnp.where(row8 >= 4, pltpu.roll(e, 4, 0), 0.0)

    def all_sent(buf, which):
        n = buf.shape[0]
        pltpu.make_async_copy(buf.at[pl.ds(0, n - 1)], buf.at[pl.ds(0, n - 1)], ar_send.at[which]).wait()

    all_to_one(packed, ar1, mx, line, 0)

    loads[5].wait()
    route()
    pl.semaphore_wait(ready, len(line))
    exchange(tx, rx)
    loads[6].wait()
    prev_halo = send_halo(1, prev, *inner, 0)
    all_to_one(all_arrived(ar1, 0), ar2, my * ngz + mz, layer, 1)
    loads[7].wait()
    loads[8].wait()
    inv[...] = 1.0 / (6.0 + idiag[...])
    v = prev[...]
    p1[...] = source[...] + near_sum(v, iy)
    for c in prev_halo:
        c.wait_recv()
    p1[...] += far_sum(v.shape, hx_i[0], hy_i[0], hz_i[0], at_ends)

    mu_rows = all_arrived(ar2, 1)
    mu = [(mu_rows[k : k + 1], mu_rows[4 + k : 5 + k]) for k in range(4)]
    a0 = mu[0][0] / mu[1][0]
    rr1 = dd_add(mu[0], dd_times(dd_add(dd_times(mu[2], a0), (-2.0 * mu[1][0], -2.0 * mu[1][1])), a0))
    rr1 = rr1[0] + rr1[1]
    beta = rr1 / mu[0][0]
    g = 1.0 + beta
    curve = dd_times(dd_add(dd_times(mu[1], g), dd_times(mu[2], -2.0 * a0)), g)
    curve = dd_add(curve, dd_times(dd_times(mu[3], a0), a0))
    a1 = rr1 / (curve[0] + curve[1])
    c0, c1 = (a0 + a1 * g)[:, :1], (-a0 * a1)[:, :1]
    a0, a1, beta = a0[:, :1], a1[:, :1], beta[:, :1]

    scatter(c0, c1)
    added = acc[pl.ds(0, ni)] + acc[pl.ds(ni, ni)]
    p1[...] = (p1[...] + added) * inv[...]
    last = send_halo(3, p1, *inner, 1)
    r, q = right[...], q0[...]
    r1 = r - a0 * q
    x_out[...] = a0 * r + a1 * (r1 + beta * r)
    res_out[...] = r1 - a1 * ((q - a0 * q1[...]) + beta * q)
    near = source[...] + added + near_sum(p1[...], iy)
    for c in last:
        c.wait_recv()
    p_out[...] = (near + far_sum(near.shape, hx_i[1], hy_i[1], hz_i[1], at_ends)) * inv[...]
    for c in first + prev_halo + second + last:
        c.wait_send()
    exchange_sent(tx)
    all_sent(ar1, 0)
    all_sent(ar2, 1)


def hand_out(x, res, p, x_hbm, res_hbm, p_hbm, sem):
    pairs = ((p, p_hbm), (x, x_hbm), (res, res_hbm))
    copies = [pltpu.make_async_copy(a, b, sem.at[i]) for i, (a, b) in enumerate(pairs)]
    for c in copies:
        c.start()
    for c in copies:
        c.wait()


def solution(mesh):
    ngx, ngy, ngz = (mesh.shape[a] for a in ("gx", "gy", "gz"))
    groups = ngx * ngy

    def per_device(right, odiag, nodes, weights, dest, cell, prev, source, idiag):
        cx, cy, nz = right.shape
        ix, iy, nzi = source.shape
        points = nodes.shape[0]
        cap = 2 * points // groups
        no, ni = cx * cy, ix * iy
        v = pltpu.VMEM
        dma = pltpu.SemaphoreType.DMA
        scratch = [
            v((no, nz), F32), v((no, nz), F32), v((1, points), I32), v((8, points), F32), v((1, points), I32),
            v((1, points), I32), v((ni, nzi), F32), v((ni, nzi), F32), v((ni, nzi), F32), dma((9,)),
            v((no, nz), F32), v((no, nz), F32), v((ni, nzi), F32),
            v((2, 2, cy, nz), F32), v((2, 2, cx, nz), F32), v((2, 2, 8, LANE), F32), v((2, 2, cx, nz), F32), v((2, 2, 8, LANE), F32),
            v((2, 2, iy, nzi), F32), v((2, 2, ix, nzi), F32), v((2, 2, 8, LANE), F32), v((2, 2, ix, nzi), F32), v((2, 2, 8, LANE), F32),
            dma((4, 6)), dma((4, 6)),
            v((ngx, 8, LANE), F32), v((ngy * ngz, 8, LANE), F32), dma((2,)), dma((2,)),
            v((groups, 1, 3 * cap), F32), v((groups, 1, 3 * cap), F32), dma(()), dma((4,)), pltpu.SemaphoreType.REGULAR,
            v((1, points), F32), v((groups, BLK), F32), v((4 * no, nz), BF16), v((1, points), F32), v((1, points), F32),
            v((6 * groups, cap), F32), v((2 * ni, nzi), F32), v((ni, nzi), F32),
        ]
        x, res, p = pl.pallas_call(
            functools.partial(kernel, (ngx, ngy, ngz, cy, iy)),
            out_shape=(v((no, nz), F32), v((no, nz), F32), v((ni, nzi), F32)),
            in_specs=[pl.BlockSpec(memory_space=pl.ANY)] * 9,
            out_specs=[pl.BlockSpec(memory_space=pltpu.VMEM)] * 3,
            scratch_shapes=scratch,
            compiler_params=pltpu.CompilerParams(
                collective_id=0, has_side_effects=True, vmem_limit_bytes=56 * 2**20
            ),
        )(
            right.reshape(no, nz), odiag.reshape(no, nz), nodes.reshape(1, points), weights,
            dest.reshape(1, points), cell.reshape(1, points), prev.reshape(ni, nzi),
            source.reshape(ni, nzi), idiag.reshape(ni, nzi),
        )
        x, res, p = pl.pallas_call(
            hand_out,
            out_shape=tuple(jax.ShapeDtypeStruct(a.shape, F32) for a in (x, res, p)),
            in_specs=[pl.BlockSpec(memory_space=pltpu.VMEM)] * 3,
            out_specs=[pl.BlockSpec(memory_space=pl.ANY)] * 3,
            scratch_shapes=[dma((3,))],
            compiler_params=pltpu.CompilerParams(vmem_limit_bytes=32 * 2**20),
        )(x, res, p)
        return x.reshape(cx, cy, nz), res.reshape(cx, cy, nz), p.reshape(ix, iy, nzi)

    block = P("gx", "gy", "gz")
    every = ("gx", "gy", "gz")
    return jax.shard_map(
        per_device,
        mesh=mesh,
        in_specs=(block, block, P(every), P(None, every), P(every, None), P(every), block, block, block),
        out_specs=(block, block, block),
        check_vma=False,
    )
```
